32 devices in a mesh: data: 2 (over x), pp: 4 (over z), ep: 4 (over y, core).
Axes of the slice: x: 2, y: 2, z: 4, core: 2. Of those that a mesh axis runs over, the one named last changes fastest.
Arguments:
- expert_out: bfloat16 [4, 4, 512, 32, 2048], P('pp', 'data', 'ep'), parts along dimension 1
- expert_ids: int32 [4, 4, 4, 256, 10], P('pp', 'data', 'ep'), parts along dimension 1
- slot_ids: int32 [4, 4, 4, 256, 10], P('pp', 'data', 'ep'), parts along dimension 1
- gate_weights: float32 [4, 4, 4, 256, 10], P('pp', 'data', 'ep'), parts along dimension 1
- residual: bfloat16 [4, 4, 4, 256, 2048], P('pp', 'data', 'ep'), parts along dimension 1
- norm_moe: float32 [4, 2048], P('pp')
- w_gate: bfloat16 [4, 2048, 512], P('pp')
- w_up: bfloat16 [4, 2048, 512], P('pp')
- w_down: bfloat16 [4, 512, 2048], P('pp')
- norm_attn: float32 [4, 2048], P('pp')
- w_query: bfloat16 [4, 2048, 16, 256], P('pp')
- w_key: bfloat16 [4, 2048, 16, 256], P('pp')
- w_value: bfloat16 [4, 2048, 16, 256], P('pp')
- w_out: bfloat16 [4, 16, 256, 2048], P('pp')
Outputs:
- output: bfloat16 [4, 4, 4, 256, 2048], P('pp', 'data', 'ep'), parts along dimension 1
There are 2 independent parts. The reference program is written for one: setup_inputs(seed, part) draws one part's arguments, and reference() takes and returns one part's arrays. A program takes and returns all parts, laid end to end along the dimension named above; an argument that names none is the same for every part.
All inputs are finite; a program needn't handle non-finite values.
Results may differ from the reference program's by a relative error of at most 0.0163687.
Values are sent between devices in bfloat16 or wider.
A program may use at most 1 GiB of HBM per device.

```python
import math
import jax
import jax.numpy as jnp
from jax import lax

STAGES = 4
EP_SIZE = 4
MICRO_BATCHES = 2
SEQ_DEV = 1
SEQ_LEN = 256
D_MODEL = 2048
NUM_HEADS = 16
HEAD_DIM = 256
EXPERTS = 512
TOP_K = 10
FF_SHARED = 512
CAP_SLOTS = 8

SEQS = EP_SIZE * SEQ_DEV
TOK_DEV = SEQ_DEV * SEQ_LEN
TOKENS = SEQS * SEQ_LEN
SLOTS = EP_SIZE * CAP_SLOTS
HEADS_WIDTH = NUM_HEADS * HEAD_DIM
SCORE_SCALE = 1.0 / math.sqrt(HEAD_DIM)
EPSILON = 1e-6


def route_group(group_args):
    group_key, hot_draw = group_args
    hot_rank = jnp.argsort(jnp.argsort(hot_draw * EXPERTS + jnp.arange(EXPERTS)))
    lead_mask = (jnp.arange(TOK_DEV) <= CAP_SLOTS).astype(jnp.int32)[:, None]
    hot_bias = jnp.where(hot_rank < max(1, TOP_K // 4), 1024, 0) + jnp.where(hot_rank == 0, 8192, 0) * lead_mask
    noise_draw = jax.random.randint(group_key, (EP_SIZE, TOK_DEV, EXPERTS), 0, 4096)
    scores = (noise_draw + hot_bias) * EXPERTS + jnp.arange(EXPERTS)
    top_vals, expert_ids = lax.top_k(scores, TOP_K)
    choice_count = TOK_DEV * TOP_K
    flat_ids = expert_ids.reshape(EP_SIZE, choice_count)
    position = jnp.arange(choice_count)
    sort_order = jnp.argsort(flat_ids * choice_count + position, axis=-1)
    sorted_ids = jnp.take_along_axis(flat_ids, sort_order, axis=-1)
    is_start = jnp.concatenate([jnp.ones((EP_SIZE, 1), jnp.bool_), sorted_ids[:, 1:] != sorted_ids[:, :-1]], axis=1)
    start_pos = lax.cummax(jnp.where(is_start, position, 0), axis=1)
    slot_rank = jnp.take_along_axis(position - start_pos, jnp.argsort(sort_order, axis=-1), axis=-1)
    source = jnp.arange(EP_SIZE)[:, None]
    slot_ids = jnp.where(slot_rank < CAP_SLOTS, source * CAP_SLOTS + slot_rank, -1)
    return expert_ids.reshape(SEQS, SEQ_LEN, TOP_K), slot_ids.reshape(SEQS, SEQ_LEN, TOP_K)


def draw_routing(key):
    key_hot, key_score = jax.random.split(key)
    hot_draw = jax.random.randint(key_hot, (STAGES * MICRO_BATCHES, EXPERTS), 0, 1 << 20)
    group_keys = jax.random.split(key_score, STAGES * MICRO_BATCHES)
    expert_ids, slot_ids = lax.map(route_group, (group_keys, hot_draw))
    route_shape = (STAGES, MICRO_BATCHES, SEQS, SEQ_LEN, TOP_K)
    return expert_ids.reshape(route_shape), slot_ids.reshape(route_shape)


def setup_inputs(seed: int = 0, part: int = 0) -> dict:
    base_key = jax.random.key(seed)
    part_keys = jax.random.split(jax.random.fold_in(base_key, part), 5)
    expert_ids, slot_ids = draw_routing(part_keys[0])
    route_shape = (STAGES, MICRO_BATCHES, SEQS, SEQ_LEN, TOP_K)
    gate_draw = jax.random.normal(part_keys[1], route_shape, jnp.float32)
    gate_weights = jnp.exp(1.2 * gate_draw - 0.72) / TOP_K
    expert_scale = jax.random.uniform(part_keys[2], (STAGES * MICRO_BATCHES, EXPERTS, 1, 1), jnp.float32, 0.5, 3.0)
    out_keys = jax.random.split(part_keys[3], STAGES * MICRO_BATCHES)

    def draw_outputs(group_args):
        group_key, group_scale = group_args
        normal_draw = jax.random.normal(group_key, (EXPERTS, SLOTS, D_MODEL), jnp.float32)
        return (normal_draw * group_scale).astype(jnp.bfloat16)

    expert_out = lax.map(draw_outputs, (out_keys, expert_scale)).reshape(STAGES, MICRO_BATCHES, EXPERTS, SLOTS, D_MODEL)
    residual = jax.random.normal(part_keys[4], (STAGES, MICRO_BATCHES, SEQS, SEQ_LEN, D_MODEL), jnp.float32).astype(jnp.bfloat16)
    weight_keys = jax.random.split(jax.random.key(seed + 1), 9)
    in_scale = 1.0 / math.sqrt(D_MODEL)
    down_scale = 2.0 / math.sqrt(FF_SHARED)
    query_scale = 1.5 / math.sqrt(D_MODEL)
    out_scale = math.sqrt(math.sqrt(SEQ_LEN)) / math.sqrt(HEADS_WIDTH)
    norm_moe = jax.random.uniform(weight_keys[0], (STAGES, D_MODEL), jnp.float32, 0.5, 1.5)
    w_gate = (jax.random.normal(weight_keys[1], (STAGES, D_MODEL, FF_SHARED), jnp.float32) * in_scale).astype(jnp.bfloat16)
    w_up = (jax.random.normal(weight_keys[2], (STAGES, D_MODEL, FF_SHARED), jnp.float32) * in_scale).astype(jnp.bfloat16)
    w_down = (jax.random.normal(weight_keys[3], (STAGES, FF_SHARED, D_MODEL), jnp.float32) * down_scale).astype(jnp.bfloat16)
    norm_attn = jax.random.uniform(weight_keys[4], (STAGES, D_MODEL), jnp.float32, 0.5, 1.5)
    w_query = (jax.random.normal(weight_keys[5], (STAGES, D_MODEL, NUM_HEADS, HEAD_DIM), jnp.float32) * query_scale).astype(jnp.bfloat16)
    w_key = (jax.random.normal(weight_keys[6], (STAGES, D_MODEL, NUM_HEADS, HEAD_DIM), jnp.float32) * in_scale).astype(jnp.bfloat16)
    w_value = (jax.random.normal(weight_keys[7], (STAGES, D_MODEL, NUM_HEADS, HEAD_DIM), jnp.float32) * in_scale).astype(jnp.bfloat16)
    w_out = (jax.random.normal(weight_keys[8], (STAGES, NUM_HEADS, HEAD_DIM, D_MODEL), jnp.float32) * out_scale).astype(jnp.bfloat16)
    return {"expert_out": expert_out, "expert_ids": expert_ids, "slot_ids": slot_ids, "gate_weights": gate_weights, "residual": residual, "norm_moe": norm_moe, "w_gate": w_gate, "w_up": w_up, "w_down": w_down, "norm_attn": norm_attn, "w_query": w_query, "w_key": w_key, "w_value": w_value, "w_out": w_out}


def rms_norm(tensor, gain):
    values = tensor.astype(jnp.float32)
    inv_rms = lax.rsqrt(jnp.mean(values * values, axis=-1, keepdims=True) + EPSILON)
    return values * inv_rms * gain


def shared_expert(residual, norm_moe, w_gate, w_up, w_down):
    normed = rms_norm(residual, norm_moe).astype(jnp.bfloat16)
    gate_act = jnp.dot(normed, w_gate, preferred_element_type=jnp.float32)
    up_act = jnp.dot(normed, w_up, preferred_element_type=jnp.float32)
    hidden = (jax.nn.silu(gate_act) * up_act).astype(jnp.bfloat16)
    return jnp.dot(hidden, w_down, preferred_element_type=jnp.float32).astype(jnp.bfloat16)


def combine_micro(micro_args, stage_weights):
    expert_out, expert_ids, slot_ids, gate_weights, residual = micro_args
    norm_moe, w_gate, w_up, w_down = stage_weights
    flat_slots = slot_ids.reshape(TOKENS, TOP_K)
    kept_mask = flat_slots >= 0
    row_ids = expert_ids.reshape(TOKENS, TOP_K) * SLOTS + jnp.where(kept_mask, flat_slots, 0)
    picked = jnp.take(expert_out.reshape(EXPERTS * SLOTS, D_MODEL), row_ids, axis=0)
    weights = jnp.where(kept_mask, gate_weights.reshape(TOKENS, TOP_K), 0.0)
    routed = jnp.sum(picked.astype(jnp.float32) * weights[:, :, None], axis=1)
    flat_resid = residual.reshape(TOKENS, D_MODEL)
    shared = shared_expert(flat_resid, norm_moe, w_gate, w_up, w_down)
    combined = flat_resid.astype(jnp.float32) + shared.astype(jnp.float32) + routed
    return combined.astype(jnp.bfloat16).reshape(SEQS, SEQ_LEN, D_MODEL)


def attend_sequence(seq_args):
    queries, key_heads, value_heads = seq_args
    scores = jnp.einsum("qhe,khe->hqk", queries.astype(jnp.float32), key_heads.astype(jnp.float32)) * SCORE_SCALE
    causal = jnp.arange(SEQ_LEN)[:, None] >= jnp.arange(SEQ_LEN)[None, :]
    scores = jnp.where(causal, scores, -1e30)
    attn_probs = jnp.exp(scores - jnp.max(scores, axis=-1, keepdims=True))
    prob_sum = jnp.sum(attn_probs, axis=-1, keepdims=True)
    attn_mixed = jnp.einsum("hqk,khe->hqe", attn_probs.astype(jnp.bfloat16).astype(jnp.float32), value_heads.astype(jnp.float32))
    return attn_mixed / prob_sum


def attention_stage(stage_args):
    received, norm_attn, w_query, w_key, w_value, w_out = stage_args
    seq_count = MICRO_BATCHES * SEQS
    normed = rms_norm(received, norm_attn).astype(jnp.bfloat16).reshape(seq_count * SEQ_LEN, D_MODEL)

    def project(weight):
        product = jnp.dot(normed, weight.reshape(D_MODEL, HEADS_WIDTH), preferred_element_type=jnp.float32)
        return product.astype(jnp.bfloat16).reshape(seq_count, SEQ_LEN, NUM_HEADS, HEAD_DIM)

    attn_mixed = lax.map(attend_sequence, (project(w_query), project(w_key), project(w_value)))
    mixed_rows = jnp.transpose(attn_mixed.astype(jnp.bfloat16), (0, 2, 1, 3)).reshape(seq_count * SEQ_LEN, HEADS_WIDTH)
    attn_proj = jnp.dot(mixed_rows, w_out.reshape(HEADS_WIDTH, D_MODEL), preferred_element_type=jnp.float32).astype(jnp.bfloat16)
    updated = received.astype(jnp.float32) + attn_proj.astype(jnp.float32).reshape(received.shape)
    return updated.astype(jnp.bfloat16)


def reference(expert_out, expert_ids, slot_ids, gate_weights, residual, norm_moe, w_gate, w_up, w_down, norm_attn, w_query, w_key, w_value, w_out):
    def combine_stage(stage_args):
        def one_micro(micro_args):
            return combine_micro(micro_args, stage_args[5:])
        return lax.map(one_micro, stage_args[:5])

    combined = lax.map(combine_stage, (expert_out, expert_ids, slot_ids, gate_weights, residual, norm_moe, w_gate, w_up, w_down))
    received = jnp.roll(combined, 1, axis=0)
    return lax.map(attention_stage, (received, norm_attn, w_query, w_key, w_value, w_out))
```

```python
import functools

import jax
import jax.numpy as jnp
from jax import lax
from jax.experimental import pallas as pl
from jax.experimental.pallas import tpu as pltpu
from jax.sharding import PartitionSpec as P

EPSILON = 1e-6
MESH = pl.DeviceIdType.MESH
F32, BF16 = jnp.float32, jnp.bfloat16
BF16_MAX = 3.3895313892515355e38
META_ROWS = 32
GATE_ROW = 16


def boundary_kernel(dims, meta, rows_hbm, resid_hbm, norm_moe, norm_attn, wg_hbm, wu_hbm, wd_hbm, wq_hbm, wk_hbm, wv_hbm, wo_hbm,
                    out_hbm, wrel_hbm,
                    meta_all, meta_cols, send_part, recv_part, mine, y_recv, recv_own, acc, y_send, y_in, resid,
                    meta_ss, meta_rs, part_ss, part_rs, own_ss, own_rs, y_ss, y_rs, z_ss, z_rs, row_sem, misc_sem, w_sem, o_sem, rl_in, rl_out):
    micro, seq, model, heads, head_dim, local_experts, cap, top_k, ff, stages = dims
    local_cols = local_experts * cap
    half = seq // 2
    piece = 32
    pieces = seq // piece
    per_half = half // piece

    me = lax.axis_index("ep")
    stage = lax.axis_index("pp")
    chip, core = me // 2, me % 2
    partner = chip * 2 + (1 - core)
    across = (1 - chip) * 2 + core
    diag = (1 - chip) * 2 + (1 - core)
    nxt, prv = (stage + 1) % stages, (stage + stages - 1) % stages

    barrier = pltpu.get_barrier_semaphore()
    for peer in (partner, across, diag):
        pl.semaphore_signal(barrier, inc=1, device_id={"ep": peer}, device_id_type=MESH)
    for peer in (nxt, prv):
        pl.semaphore_signal(barrier, inc=1, device_id={"pp": peer}, device_id_type=MESH)
    pl.semaphore_wait(barrier, 5)

    def meta_copy(rel, peer):
        return pltpu.make_async_remote_copy(src_ref=meta, dst_ref=meta_all.at[rel - 1], send_sem=meta_ss.at[rel - 1], recv_sem=meta_rs.at[rel - 1], device_id={"ep": peer}, device_id_type=MESH)

    def part_copy(m, c):
        sl = pl.ds(pl.multiple_of(c * half, half), half)
        return pltpu.make_async_remote_copy(src_ref=send_part.at[m, sl], dst_ref=recv_part.at[m, sl], send_sem=part_ss.at[m, c], recv_sem=part_rs.at[m, c], device_id={"ep": partner}, device_id_type=MESH)

    def own_copy(m, c):
        sl = pl.ds(pl.multiple_of(c * half, half), half)
        return pltpu.make_async_remote_copy(src_ref=send_part.at[m, sl], dst_ref=recv_own.at[m, sl], send_sem=own_ss.at[m, c], recv_sem=own_rs.at[m, c], device_id={"ep": partner}, device_id_type=MESH)

    def y_copy(m, k):
        sl = pl.ds(pl.multiple_of(k * piece, piece), piece)
        return pltpu.make_async_remote_copy(src_ref=mine.at[m, sl], dst_ref=y_recv.at[m, sl], send_sem=y_ss.at[m, k], recv_sem=y_rs.at[m, k], device_id={"ep": across}, device_id_type=MESH)

    def z_copy(m, k):
        sl = pl.ds(pl.multiple_of(k * piece, piece), piece)
        return pltpu.make_async_remote_copy(src_ref=y_send.at[m, sl], dst_ref=y_in.at[m, sl], send_sem=z_ss.at[m, k], recv_sem=z_rs.at[m, k], device_id={"pp": nxt}, device_id_type=MESH)

    for rel, peer in ((2, across), (3, diag), (1, partner)):
        meta_copy(rel, peer).start()

    def phase_one(rbuf, wbuf, wg, wu, wd, xs, hid):
        def rows_copy(p, ab):
            m = p % 2
            far = 1 - p // 2
            owner_a = far * diag + (1 - far) * partner
            owner_b = far * across + (1 - far) * me
            owner = owner_a if ab == 0 else owner_b
            src = rows_hbm.at[m, :, pl.ds(pl.multiple_of(owner * cap, cap), cap), :]
            return pltpu.make_async_copy(src, rbuf.at[p % 2, ab], row_sem.at[p % 2, ab])

        rows_copy(0, 0).start()
        rows_copy(0, 1).start()
        res_cp = pltpu.make_async_copy(resid_hbm, resid, misc_sem.at[0])
        wg_cp = pltpu.make_async_copy(wg_hbm, wg, misc_sem.at[1])
        wu_cp = pltpu.make_async_copy(wu_hbm, wu, misc_sem.at[2])
        wd_cp = pltpu.make_async_copy(wd_hbm, wd, misc_sem.at[3])
        for cp in (res_cp, wg_cp, wu_cp, wd_cp):
            cp.start()

        for m in range(micro):
            meta_cols[0, m] = meta[m].T
        for rel, peer in ((2, across), (3, diag), (1, partner)):
            meta_copy(rel, peer).wait()
            for m in range(micro):
                meta_cols[rel, m] = meta_all[rel - 1, m].T

        base = (local_cols * me).astype(F32)
        lane = lax.broadcasted_iota(jnp.int32, (half, 256), 1).astype(F32) + base

        def partial_sum(p, c, ab, dst):
            m = p % 2
            far = 1 - p // 2
            rel = (1 + 2 * far) if ab == 0 else 2 * far
            tok = pl.ds(pl.multiple_of(c * half, half), half)
            table = meta_cols[rel, m, tok, :]

            def build(kb, carry):
                col_id = lane + (kb * 256).astype(F32)
                w = jnp.zeros((half, 256), F32)
                for j in range(top_k):
                    w = jnp.where(table[:, j:j + 1] == col_id, table[:, GATE_ROW + j:GATE_ROW + j + 1], w)
                hi = jnp.minimum(w, BF16_MAX).astype(BF16)
                rest = w - hi.astype(F32)
                mid = rest.astype(BF16)
                low = (rest - mid.astype(F32)).astype(BF16)
                kk = pl.ds(pl.multiple_of(kb * 256, 256), 256)
                wbuf[ab, 0:half, kk] = hi
                wbuf[ab, half:2 * half, kk] = mid
                wbuf[ab, 2 * half:3 * half, kk] = low
                return carry

            lax.fori_loop(0, local_cols // 256, build, 0)

            def mul(n, carry):
                nn = pl.ds(pl.multiple_of(n * 512, 512), 512)
                rr = rbuf[p % 2, ab, :, :, nn].reshape(local_cols, 512)
                d = jnp.dot(wbuf[ab], rr, preferred_element_type=F32)
                dst[m, tok, nn] = d[0:half] + d[half:2 * half] + d[2 * half:3 * half]
                return carry

            lax.fori_loop(0, model // 512, mul, 0)

        def pair_step(q, carry):
            p, c = q // 2, q % 2
            m = p % 2

            @pl.when(c == 0)
            def _():
                rows_copy(p, 0).wait()
                rows_copy(p, 1).wait()

                @pl.when(p < 3)
                def _():
                    rows_copy(p + 1, 0).start()
                    rows_copy(p + 1, 1).start()

            @pl.when(p >= 2)
            def _():
                part_copy(m, c).wait_send()

            partial_sum(p, c, 0, send_part)

            @pl.when(p < 2)
            def _():
                part_copy(m, c).start()

            @pl.when(p >= 2)
            def _():
                own_copy(m, c).start()

            @pl.when(p < 2)
            def _():
                partial_sum(p, c, 1, mine)
                part_copy(m, c).wait_recv()

                def add(k, carry):
                    sl = pl.ds(pl.multiple_of(k * piece, piece), piece)
                    mine[m, sl] = mine[m, sl] + recv_part[m, sl]
                    y_copy(m, k).start()
                    return carry

                lax.fori_loop(c * per_half, (c + 1) * per_half, add, 0)

            @pl.when(p >= 2)
            def _():
                partial_sum(p, c, 1, acc)
            return carry

        lax.fori_loop(0, 8, pair_step, 0)

        for cp in (res_cp, wg_cp, wu_cp, wd_cp):
            cp.wait()

        def shared(m, carry):
            def norm(k, carry):
                sl = pl.ds(pl.multiple_of(k * piece, piece), piece)
                v = resid[m, sl].astype(F32)
                inv = lax.rsqrt(jnp.mean(v * v, axis=-1, keepdims=True) + EPSILON)
                xs[sl] = (v * inv * norm_moe[...]).astype(BF16)
                return carry

            lax.fori_loop(0, pieces, norm, 0)

            def up(n, carry):
                nn = pl.ds(pl.multiple_of(n * 256, 256), 256)
                g = jnp.dot(xs[...], wg[:, nn], preferred_element_type=F32)
                u = jnp.dot(xs[...], wu[:, nn], preferred_element_type=F32)
                hid[:, nn] = (g * (1.0 / (1.0 + jnp.exp(-g))) * u).astype(BF16)
                return carry

            lax.fori_loop(0, ff // 256, up, 0)
            for c in range(2):
                own_copy(m, c).wait()

            def down(n, carry):
                nn = pl.ds(pl.multiple_of(n * 256, 256), 256)
                s = jnp.dot(hid[...], wd[:, nn], preferred_element_type=F32).astype(BF16)
                acc[m, :, nn] = (resid[m, :, nn].astype(F32) + s.astype(F32)) + (acc[m, :, nn] + recv_own[m, :, nn])
                return carry

            lax.fori_loop(0, model // 256, down, 0)
            return carry

        lax.fori_loop(0, micro, shared, 0)

    pl.run_scoped(
        phase_one,
        pltpu.VMEM((2, 2, local_experts, cap, model), BF16),
        pltpu.VMEM((2, 3 * half, local_cols), BF16),
        pltpu.VMEM((model, ff), BF16),
        pltpu.VMEM((model, ff), BF16),
        pltpu.VMEM((ff, model), BF16),
        pltpu.VMEM((seq, model), BF16),
        pltpu.VMEM((seq, ff), BF16),
    )

    def finish(m, lo, hi):
        def body(k, carry):
            sl = pl.ds(pl.multiple_of(k * piece, piece), piece)
            y_copy(m, k).wait()
            y_send[m, sl] = (acc[m, sl] + y_recv[m, sl]).astype(BF16)
            z_copy(m, k).start()
            return carry

        lax.fori_loop(lo, hi, body, 0)

    def phase_two(rin, rout, wbuf, obuf, wob, xbuf, mixed):
        d_blk = 64
        sub = 256 // heads
        blocks = model // d_blk
        row = lax.broadcasted_iota(jnp.int32, (256, 256), 0)
        col = lax.broadcasted_iota(jnp.int32, (256, 256), 1)
        pick = jnp.where(col == (row % sub) * heads + row // sub, 1.0, 0.0).astype(BF16)

        def relayout(mat, src_hbm):
            def in_copy(b):
                return pltpu.make_async_copy(src_hbm.at[pl.ds(pl.multiple_of(b * d_blk, d_blk), d_blk)], rin.at[b % 2], rl_in.at[b % 2])

            def out_copy(b):
                return pltpu.make_async_copy(rout.at[b % 2], wrel_hbm.at[mat, :, pl.ds(pl.multiple_of(b * d_blk, d_blk), d_blk), :], rl_out.at[b % 2])

            in_copy(0).start()

            def body(b, carry):
                in_copy(b).wait()

                @pl.when(b + 1 < blocks)
                def _():
                    in_copy(b + 1).start()

                @pl.when(b >= 2)
                def _():
                    out_copy(b - 2).wait()
                for i in range(d_blk // sub):
                    tile = rin[b % 2, i * sub:(i + 1) * sub].reshape(sub * heads, head_dim)
                    moved = jnp.dot(pick, tile, preferred_element_type=F32).astype(BF16)
                    rout[b % 2, :, i * sub:(i + 1) * sub, :] = moved.reshape(heads, sub, head_dim)
                out_copy(b).start()
                return carry

            lax.fori_loop(0, blocks, body, 0)
            out_copy(blocks - 2).wait()
            out_copy(blocks - 1).wait()

        finish(0, 0, 4)
        relayout(0, wq_hbm)
        finish(0, 4, 6)
        relayout(1, wk_hbm)
        finish(0, 6, 8)
        relayout(2, wv_hbm)

        def w_copy(h, mat):
            return pltpu.make_async_copy(wrel_hbm.at[mat, h], wbuf.at[h % 2, mat], w_sem.at[h % 2, mat])

        n_out = model // 512

        def o_copy(n):
            return pltpu.make_async_copy(wo_hbm.at[:, pl.ds(pl.multiple_of(n * 512, 512), 512)], wob.at[n % 2], o_sem.at[n % 2])

        for mat in range(3):
            w_copy(0, mat).start()
        o_copy(0).start()

        qi = lax.broadcasted_iota(jnp.int32, (seq, seq), 0)
        ki = lax.broadcasted_iota(jnp.int32, (seq, seq), 1)
        causal = qi >= ki
        scale = 1.0 / (head_dim ** 0.5)

        def attention(m):
            last = m == micro - 1

            def norm(k, carry):
                sl = pl.ds(pl.multiple_of(k * piece, piece), piece)
                z_copy(m, k).wait()
                v = y_in[m, sl].astype(F32)
                inv = lax.rsqrt(jnp.mean(v * v, axis=-1, keepdims=True) + EPSILON)
                xbuf[sl] = (v * inv * norm_attn[...]).astype(BF16)
                return carry

            lax.fori_loop(0, pieces, norm, 0)

            def head(h, carry):
                slot = h % 2
                for mat in range(3):
                    w_copy(h, mat).wait()

                def prefetch():
                    for mat in range(3):
                        w_copy((h + 1) % heads, mat).start()

                if last:
                    pl.when(h + 1 < heads)(prefetch)
                else:
                    prefetch()
                x = xbuf[...]
                q = jnp.dot(x, wbuf[slot, 0], preferred_element_type=F32).astype(BF16)
                k = jnp.dot(x, wbuf[slot, 1], preferred_element_type=F32).astype(BF16)
                v = jnp.dot(x, wbuf[slot, 2], preferred_element_type=F32).astype(BF16)
                s = lax.dot_general(q, k, (((1,), (1,)), ((), ())), preferred_element_type=F32) * scale
                s = jnp.where(causal, s, -1e30)
                e = jnp.exp(s - jnp.max(s, axis=-1, keepdims=True))
                total = jnp.sum(e, axis=-1, keepdims=True)
                o = jnp.dot(e.astype(BF16), v, preferred_element_type=F32) / total
                mixed[:, pl.ds(pl.multiple_of(h * head_dim, head_dim), head_dim)] = o.astype(BF16)
                if not last:
                    @pl.when((h % 4 == 0) & (h > 0))
                    def _():
                        finish(1, h // 4 + 1, h // 4 + 2)
                return carry

            lax.fori_loop(0, heads, head, 0)

            def proj(n, carry):
                nn = pl.ds(pl.multiple_of(n * 512, 512), 512)
                o_copy(n).wait()
                if last:
                    pl.when(n + 1 < n_out)(lambda: o_copy(n + 1).start())
                else:
                    o_copy((n + 1) % n_out).start()
                pr = jnp.dot(mixed[...], wob[n % 2], preferred_element_type=F32).astype(BF16)
                obuf[m, :, nn] = (y_in[m, :, nn].astype(F32) + pr.astype(F32)).astype(BF16)
                return carry

            lax.fori_loop(0, n_out, proj, 0)
            pltpu.make_async_copy(obuf.at[m], out_hbm.at[m], misc_sem.at[4 + m]).start()

        finish(1, 0, 2)
        attention(0)
        finish(1, 5, 8)
        attention(1)
        for m in range(micro):
            pltpu.make_async_copy(obuf.at[m], out_hbm.at[m], misc_sem.at[4 + m]).wait()

    pl.run_scoped(
        phase_two,
        pltpu.VMEM((2, 64, heads, head_dim), BF16),
        pltpu.VMEM((2, heads, 64, head_dim), BF16),
        pltpu.VMEM((2, 3, model, head_dim), BF16),
        pltpu.VMEM((micro, seq, model), BF16),
        pltpu.VMEM((2, heads * head_dim, 512), BF16),
        pltpu.VMEM((seq, model), BF16),
        pltpu.VMEM((seq, heads * head_dim), BF16),
    )


def solution(mesh):
    stages = mesh.shape["pp"]
    ep_size = mesh.shape["ep"]
    tok_spec = P("pp", "data", "ep", None, None)
    vec_spec = P("pp", None)
    mat_spec = P("pp", None, None)
    head_spec = P("pp", None, None, None)

    def device_step(expert_out, expert_ids, slot_ids, gate_weights, residual, norm_moe, w_gate, w_up, w_down, norm_attn, w_query, w_key, w_value, w_out):
        micro = expert_out.shape[1]
        local_experts, slots_total, model = expert_out.shape[2:]
        cap = slots_total // ep_size
        seq, top_k = expert_ids.shape[3:]
        heads, head_dim = w_query.shape[2:]
        ff = w_gate.shape[2]
        ids = jnp.swapaxes(expert_ids[0, :, 0], 1, 2)
        slots = jnp.swapaxes(slot_ids[0, :, 0], 1, 2)
        gates = jnp.swapaxes(gate_weights[0, :, 0], 1, 2)
        kept = slots >= 0
        cols = jnp.where(kept, ids * cap + (slots - lax.axis_index("ep") * cap), -1).astype(F32)
        gates = jnp.where(kept, gates, 0.0)
        gap = ((0, 0), (0, GATE_ROW - top_k), (0, 0))
        meta = jnp.concatenate([jnp.pad(cols, gap), jnp.pad(gates, gap)], axis=1)

        dims = (micro, seq, model, heads, head_dim, local_experts, cap, top_k, ff, stages)
        hbm = pl.BlockSpec(memory_space=pl.ANY)
        vmem = pl.BlockSpec(memory_space=pltpu.VMEM)
        dma = pltpu.SemaphoreType.DMA
        pieces = seq // 32
        out, _ = pl.pallas_call(
            functools.partial(boundary_kernel, dims),
            out_shape=(jax.ShapeDtypeStruct((micro, seq, model), BF16), jax.ShapeDtypeStruct((3, heads, model, head_dim), BF16)),
            in_specs=[vmem, hbm, hbm, vmem, vmem] + [hbm] * 7,
            out_specs=(hbm, hbm),
            scratch_shapes=[
                pltpu.VMEM((3, micro, META_ROWS, seq), F32),
                pltpu.VMEM((4, micro, seq, META_ROWS), F32),
                pltpu.VMEM((micro, seq, model), F32),
                pltpu.VMEM((micro, seq, model), F32),
                pltpu.VMEM((micro, seq, model), F32),
                pltpu.VMEM((micro, seq, model), F32),
                pltpu.VMEM((micro, seq, model), F32),
                pltpu.VMEM((micro, seq, model), F32),
                pltpu.VMEM((micro, seq, model), BF16),
                pltpu.VMEM((micro, seq, model), BF16),
                pltpu.VMEM((micro, seq, model), BF16),
                dma((3,)), dma((3,)),
                dma((micro, 2)), dma((micro, 2)),
                dma((micro, 2)), dma((micro, 2)),
                dma((micro, pieces)), dma((micro, pieces)),
                dma((micro, pieces)), dma((micro, pieces)),
                dma((2, 2)), dma((6,)), dma((2, 3)), dma((2,)), dma((2,)), dma((2,)),
            ],
            compiler_params=pltpu.CompilerParams(collective_id=0, has_side_effects=True, vmem_limit_bytes=67043328),
        )(
            meta,
            expert_out[0],
            residual[0, :, 0],
            norm_moe, norm_attn,
            w_gate[0], w_up[0], w_down[0],
            w_query[0], w_key[0], w_value[0],
            w_out[0].reshape(heads * head_dim, model),
        )
        return out[None, :, None]

    in_specs = (tok_spec,) * 5 + (vec_spec, mat_spec, mat_spec, mat_spec, vec_spec, head_spec, head_spec, head_spec, head_spec)
    return jax.shard_map(device_step, mesh=mesh, in_specs=in_specs, out_specs=tok_spec, check_vma=False)
```

```python
import functools

import jax
import jax.numpy as jnp
from jax import lax
from jax.experimental import pallas as pl
from jax.experimental.pallas import tpu as pltpu
from jax.sharding import PartitionSpec as P

EPSILON = 1e-6
MESH = pl.DeviceIdType.MESH
F32, BF16 = jnp.float32, jnp.bfloat16
BF16_MAX = 3.3895313892515355e38
META_ROWS = 48
GATE_ROW = 16
SLOT_ROW = 32
RIN, ROUT, WSLOTS, OSLOTS, OCOLS = 6, 3, 4, 4, 256


def boundary_kernel(dims, meta, rows_hbm, resid_hbm, norm_moe, norm_attn, wg_hbm, wu_hbm, wd_hbm, wq_hbm, wk_hbm, wv_hbm, wo_hbm,
                    out_hbm, wrel_hbm,
                    meta_all, meta_cols, send_part, recv_part, mine, y_recv, recv_own, acc, y_send, y_in,
                    meta_ss, meta_rs, part_ss, part_rs, own_ss, own_rs, y_ss, y_rs, z_ss, z_rs, row_sem, misc_sem, w_sem, o_sem, rl_in, rl_out):
    micro, seq, model, heads, head_dim, local_experts, cap, top_k, ff, stages = dims
    local_cols = local_experts * cap
    half = seq // 2
    piece = 32
    pieces = seq // piece
    per_half = half // piece

    me = lax.axis_index("ep")
    stage = lax.axis_index("pp")
    chip, core = me // 2, me % 2
    partner = chip * 2 + (1 - core)
    across = (1 - chip) * 2 + core
    diag = (1 - chip) * 2 + (1 - core)
    nxt, prv = (stage + 1) % stages, (stage + stages - 1) % stages

    barrier = pltpu.get_barrier_semaphore()
    for peer in (partner, across, diag):
        pl.semaphore_signal(barrier, inc=1, device_id={"ep": peer}, device_id_type=MESH)
    for peer in (nxt, prv):
        pl.semaphore_signal(barrier, inc=1, device_id={"pp": peer}, device_id_type=MESH)
    pl.semaphore_wait(barrier, 5)

    def meta_copy(rel, peer):
        return pltpu.make_async_remote_copy(src_ref=meta, dst_ref=meta_all.at[rel - 1], send_sem=meta_ss.at[rel - 1], recv_sem=meta_rs.at[rel - 1], device_id={"ep": peer}, device_id_type=MESH)

    def part_copy(m, c):
        sl = pl.ds(pl.multiple_of(c * half, half), half)
        return pltpu.make_async_remote_copy(src_ref=send_part.at[m, sl], dst_ref=recv_part.at[m, sl], send_sem=part_ss.at[m, c], recv_sem=part_rs.at[m, c], device_id={"ep": partner}, device_id_type=MESH)

    def own_copy(m, c):
        sl = pl.ds(pl.multiple_of(c * half, half), half)
        return pltpu.make_async_remote_copy(src_ref=send_part.at[m, sl], dst_ref=recv_own.at[m, sl], send_sem=own_ss.at[m, c], recv_sem=own_rs.at[m, c], device_id={"ep": partner}, device_id_type=MESH)

    def y_copy(m, k):
        sl = pl.ds(pl.multiple_of(k * piece, piece), piece)
        return pltpu.make_async_remote_copy(src_ref=mine.at[m, sl], dst_ref=y_recv.at[m, sl], send_sem=y_ss.at[m, k], recv_sem=y_rs.at[m, k], device_id={"ep": across}, device_id_type=MESH)

    def z_copy(m, k):
        sl = pl.ds(pl.multiple_of(k * piece, piece), piece)
        return pltpu.make_async_remote_copy(src_ref=y_send.at[m, sl], dst_ref=y_in.at[m, sl], send_sem=z_ss.at[m, k], recv_sem=z_rs.at[m, k], device_id={"pp": nxt}, device_id_type=MESH)

    for rel, peer in ((2, across), (3, diag), (1, partner)):
        meta_copy(rel, peer).start()

    def phase_one(rbuf, wbuf, wg, wu, wd, xs, hid, resid, spread):
        def rows_copy(p, ab):
            m = p % 2
            far = 1 - p // 2
            owner_a = far * diag + (1 - far) * partner
            owner_b = far * across + (1 - far) * me
            owner = owner_a if ab == 0 else owner_b
            src = rows_hbm.at[m, :, pl.ds(pl.multiple_of(owner * cap, cap), cap), :]
            return pltpu.make_async_copy(src, rbuf.at[p % 2, ab], row_sem.at[p % 2, ab])

        rows_copy(0, 0).start()
        rows_copy(0, 1).start()
        res_cp = pltpu.make_async_copy(resid_hbm, resid, misc_sem.at[0])
        wg_cp = pltpu.make_async_copy(wg_hbm, wg, misc_sem.at[1])
        wu_cp = pltpu.make_async_copy(wu_hbm, wu, misc_sem.at[2])
        wd_cp = pltpu.make_async_copy(wd_hbm, wd, misc_sem.at[3])
        for cp in (res_cp, wg_cp, wu_cp, wd_cp):
            cp.start()

        for m in range(micro):
            meta_cols[0, m] = meta[m].T
        for rel, peer in ((2, across), (3, diag), (1, partner)):
            meta_copy(rel, peer).wait()
            for m in range(micro):
                meta_cols[rel, m] = meta_all[rel - 1, m].T

        lane = (lax.broadcasted_iota(jnp.int32, (half, local_experts), 1) + local_experts * me).astype(F32)
        lane_slot = (lax.broadcasted_iota(jnp.int32, (half, 256), 1) % cap).astype(F32)
        from_row = lax.broadcasted_iota(jnp.int32, (local_experts, 256), 0)
        to_col = lax.broadcasted_iota(jnp.int32, (local_experts, 256), 1) // cap
        for kb in range(local_cols // 256):
            spread[kb] = jnp.where(from_row == to_col + kb * (256 // cap), 1.0, 0.0).astype(BF16)

        def partial_sum(p, c, ab, dst):
            m = p % 2
            far = 1 - p // 2
            rel = (1 + 2 * far) if ab == 0 else 2 * far
            tok = pl.ds(pl.multiple_of(c * half, half), half)
            table = meta_cols[rel, m, tok, :]

            gate = jnp.zeros((half, local_experts), F32)
            slot = jnp.zeros((half, local_experts), F32)
            for j in range(top_k):
                hit = table[:, j:j + 1] == lane
                gate = jnp.where(hit, table[:, GATE_ROW + j:GATE_ROW + j + 1], gate)
                slot = jnp.where(hit, table[:, SLOT_ROW + j:SLOT_ROW + j + 1], slot)
            hi = jnp.minimum(gate, BF16_MAX).astype(BF16)
            rest = gate - hi.astype(F32)
            mid = rest.astype(BF16)
            low = (rest - mid.astype(F32)).astype(BF16)
            packed = jnp.concatenate([slot.astype(BF16), hi, mid, low], axis=0)
            for kb in range(local_cols // 256):
                wide = jnp.dot(packed, spread[kb], preferred_element_type=F32)
                keep = wide[0:half] == lane_slot
                for part in range(3):
                    term = jnp.where(keep, wide[(part + 1) * half:(part + 2) * half], 0.0)
                    wbuf[ab, part * half:(part + 1) * half, kb * 256:(kb + 1) * 256] = term.astype(BF16)

            def mul(n, carry):
                nn = pl.ds(pl.multiple_of(n * 512, 512), 512)
                rr = rbuf[p % 2, ab, :, :, nn].reshape(local_cols, 512)
                d = jnp.dot(wbuf[ab], rr, preferred_element_type=F32)
                dst[m, tok, nn] = d[0:half] + d[half:2 * half] + d[2 * half:3 * half]
                return carry

            lax.fori_loop(0, model // 512, mul, 0)

        def pair_step(q, carry):
            p, c = q // 2, q % 2
            m = p % 2

            @pl.when(c == 0)
            def _():
                rows_copy(p, 0).wait()
                rows_copy(p, 1).wait()

                @pl.when(p < 3)
                def _():
                    rows_copy(p + 1, 0).start()
                    rows_copy(p + 1, 1).start()

            @pl.when(p >= 2)
            def _():
                part_copy(m, c).wait_send()

            partial_sum(p, c, 0, send_part)

            @pl.when(p < 2)
            def _():
                part_copy(m, c).start()

            @pl.when(p >= 2)
            def _():
                own_copy(m, c).start()

            @pl.when(p < 2)
            def _():
                partial_sum(p, c, 1, mine)
                part_copy(m, c).wait_recv()

                def add(k, carry):
                    sl = pl.ds(pl.multiple_of(k * piece, piece), piece)
                    mine[m, sl] = mine[m, sl] + recv_part[m, sl]
                    y_copy(m, k).start()
                    return carry

                lax.fori_loop(c * per_half, (c + 1) * per_half, add, 0)

            @pl.when(p >= 2)
            def _():
                partial_sum(p, c, 1, acc)
            return carry

        lax.fori_loop(0, 8, pair_step, 0)

        for cp in (res_cp, wg_cp, wu_cp, wd_cp):
            cp.wait()

        def shared(m, carry):
            def norm(k, carry):
                sl = pl.ds(pl.multiple_of(k * piece, piece), piece)
                v = resid[m, sl].astype(F32)
                inv = lax.rsqrt(jnp.mean(v * v, axis=-1, keepdims=True) + EPSILON)
                xs[sl] = (v * inv * norm_moe[...]).astype(BF16)
                return carry

            lax.fori_loop(0, pieces, norm, 0)

            def up(n, carry):
                nn = pl.ds(pl.multiple_of(n * 256, 256), 256)
                g = jnp.dot(xs[...], wg[:, nn], preferred_element_type=F32)
                u = jnp.dot(xs[...], wu[:, nn], preferred_element_type=F32)
                hid[:, nn] = (g * (1.0 / (1.0 + jnp.exp(-g))) * u).astype(BF16)
                return carry

            lax.fori_loop(0, ff // 256, up, 0)
            for c in range(2):
                own_copy(m, c).wait()

            def down(n, carry):
                nn = pl.ds(pl.multiple_of(n * 256, 256), 256)
                s = jnp.dot(hid[...], wd[:, nn], preferred_element_type=F32).astype(BF16)
                acc[m, :, nn] = (resid[m, :, nn].astype(F32) + s.astype(F32)) + (acc[m, :, nn] + recv_own[m, :, nn])
                return carry

            lax.fori_loop(0, model // 256, down, 0)
            return carry

        lax.fori_loop(0, micro, shared, 0)

    pl.run_scoped(
        phase_one,
        pltpu.VMEM((2, 2, local_experts, cap, model), BF16),
        pltpu.VMEM((2, 3 * half, local_cols), BF16),
        pltpu.VMEM((model, ff), BF16),
        pltpu.VMEM((model, ff), BF16),
        pltpu.VMEM((ff, model), BF16),
        pltpu.VMEM((seq, model), BF16),
        pltpu.VMEM((seq, ff), BF16),
        pltpu.VMEM((micro, seq, model), BF16),
        pltpu.VMEM((local_cols // 256, local_experts, 256), BF16),
    )

    def finish(m, lo, hi):
        def body(k, carry):
            sl = pl.ds(pl.multiple_of(k * piece, piece), piece)
            y_copy(m, k).wait()
            y_send[m, sl] = (acc[m, sl] + y_recv[m, sl]).astype(BF16)
            z_copy(m, k).start()
            return carry

        lax.fori_loop(lo, hi, body, 0)

    def phase_two(rin, rout, wbuf, obuf, wob, xbuf, mixed):
        d_blk = 64
        sub = 256 // heads
        blocks = model // d_blk
        row = lax.broadcasted_iota(jnp.int32, (256, 256), 0)
        col = lax.broadcasted_iota(jnp.int32, (256, 256), 1)
        pick = jnp.where(col == (row % sub) * heads + row // sub, 1.0, 0.0).astype(BF16)

        def relayout(mat, src_hbm):
            def in_copy(b):
                return pltpu.make_async_copy(src_hbm.at[pl.ds(pl.multiple_of(b * d_blk, d_blk), d_blk)], rin.at[b % RIN], rl_in.at[b % RIN])

            def out_copy(b):
                return pltpu.make_async_copy(rout.at[b % ROUT], wrel_hbm.at[mat, :, pl.ds(pl.multiple_of(b * d_blk, d_blk), d_blk), :], rl_out.at[b % ROUT])

            for b in range(RIN - 1):
                in_copy(b).start()

            def body(b, carry):
                in_copy(b).wait()

                @pl.when(b + RIN - 1 < blocks)
                def _():
                    in_copy(b + RIN - 1).start()

                @pl.when(b >= ROUT)
                def _():
                    out_copy(b - ROUT).wait()
                for i in range(d_blk // sub):
                    tile = rin[b % RIN, i * sub:(i + 1) * sub].reshape(sub * heads, head_dim)
                    moved = jnp.dot(pick, tile, preferred_element_type=F32).astype(BF16)
                    rout[b % ROUT, :, i * sub:(i + 1) * sub, :] = moved.reshape(heads, sub, head_dim)
                out_copy(b).start()
                return carry

            lax.fori_loop(0, blocks, body, 0)
            for b in range(blocks - ROUT, blocks):
                out_copy(b).wait()

        finish(0, 0, 4)
        relayout(0, wq_hbm)
        finish(0, 4, 6)
        relayout(1, wk_hbm)
        finish(0, 6, 8)
        relayout(2, wv_hbm)

        def w_copy(h, mat):
            return pltpu.make_async_copy(wrel_hbm.at[mat, h], wbuf.at[h % WSLOTS, mat], w_sem.at[h % WSLOTS, mat])

        n_out = model // OCOLS

        def o_copy(n):
            return pltpu.make_async_copy(wo_hbm.at[:, pl.ds(pl.multiple_of(n * OCOLS, OCOLS), OCOLS)], wob.at[n % OSLOTS], o_sem.at[n % OSLOTS])

        for h in range(WSLOTS - 1):
            for mat in range(3):
                w_copy(h, mat).start()
        for n in range(OSLOTS - 1):
            o_copy(n).start()

        qi = lax.broadcasted_iota(jnp.int32, (seq, seq), 0)
        ki = lax.broadcasted_iota(jnp.int32, (seq, seq), 1)
        causal = qi >= ki
        scale = 1.0 / (head_dim ** 0.5)

        def attention(m):
            last = m == micro - 1

            def norm(k, carry):
                sl = pl.ds(pl.multiple_of(k * piece, piece), piece)
                z_copy(m, k).wait()
                v = y_in[m, sl].astype(F32)
                inv = lax.rsqrt(jnp.mean(v * v, axis=-1, keepdims=True) + EPSILON)
                xbuf[sl] = (v * inv * norm_attn[...]).astype(BF16)
                return carry

            lax.fori_loop(0, pieces, norm, 0)

            def head(h, carry):
                slot = h % WSLOTS
                for mat in range(3):
                    w_copy(h, mat).wait()

                def prefetch():
                    for mat in range(3):
                        w_copy((h + WSLOTS - 1) % heads, mat).start()

                if last:
                    pl.when(h + WSLOTS - 1 < heads)(prefetch)
                else:
                    prefetch()
                x = xbuf[...]
                q = jnp.dot(x, wbuf[slot, 0], preferred_element_type=F32).astype(BF16)
                k = jnp.dot(x, wbuf[slot, 1], preferred_element_type=F32).astype(BF16)
                v = jnp.dot(x, wbuf[slot, 2], preferred_element_type=F32).astype(BF16)
                s = lax.dot_general(q, k, (((1,), (1,)), ((), ())), preferred_element_type=F32) * scale
                s = jnp.where(causal, s, -1e30)
                e = jnp.exp(s - jnp.max(s, axis=-1, keepdims=True))
                total = jnp.sum(e, axis=-1, keepdims=True)
                o = jnp.dot(e.astype(BF16), v, preferred_element_type=F32) / total
                mixed[:, pl.ds(pl.multiple_of(h * head_dim, head_dim), head_dim)] = o.astype(BF16)
                if not last:
                    @pl.when((h % 4 == 0) & (h > 0))
                    def _():
                        finish(1, h // 4 + 1, h // 4 + 2)
                return carry

            lax.fori_loop(0, heads, head, 0)

            def proj(n, carry):
                nn = pl.ds(pl.multiple_of(n * OCOLS, OCOLS), OCOLS)
                o_copy(n).wait()
                if last:
                    pl.when(n + OSLOTS - 1 < n_out)(lambda: o_copy(n + OSLOTS - 1).start())
                else:
                    o_copy((n + OSLOTS - 1) % n_out).start()
                pr = jnp.dot(mixed[...], wob[n % OSLOTS], preferred_element_type=F32).astype(BF16)
                obuf[:, nn] = (y_in[m, :, nn].astype(F32) + pr.astype(F32)).astype(BF16)
                return carry

            lax.fori_loop(0, n_out, proj, 0)
            out_cp = pltpu.make_async_copy(obuf, out_hbm.at[m], misc_sem.at[4])
            out_cp.start()
            out_cp.wait()

        finish(1, 0, 2)
        attention(0)
        finish(1, 5, 8)
        attention(1)

    pl.run_scoped(
        phase_two,
        pltpu.VMEM((RIN, 64, heads, head_dim), BF16),
        pltpu.VMEM((ROUT, heads, 64, head_dim), BF16),
        pltpu.VMEM((WSLOTS, 3, model, head_dim), BF16),
        pltpu.VMEM((seq, model), BF16),
        pltpu.VMEM((OSLOTS, heads * head_dim, OCOLS), BF16),
        pltpu.VMEM((seq, model), BF16),
        pltpu.VMEM((seq, heads * head_dim), BF16),
    )


def solution(mesh):
    stages = mesh.shape["pp"]
    ep_size = mesh.shape["ep"]
    tok_spec = P("pp", "data", "ep", None, None)
    vec_spec = P("pp", None)
    mat_spec = P("pp", None, None)
    head_spec = P("pp", None, None, None)

    def device_step(expert_out, expert_ids, slot_ids, gate_weights, residual, norm_moe, w_gate, w_up, w_down, norm_attn, w_query, w_key, w_value, w_out):
        micro = expert_out.shape[1]
        local_experts, slots_total, model = expert_out.shape[2:]
        cap = slots_total // ep_size
        seq, top_k = expert_ids.shape[3:]
        heads, head_dim = w_query.shape[2:]
        ff = w_gate.shape[2]
        ids = jnp.swapaxes(expert_ids[0, :, 0], 1, 2)
        slots = jnp.swapaxes(slot_ids[0, :, 0], 1, 2)
        gates = jnp.swapaxes(gate_weights[0, :, 0], 1, 2)
        kept = slots >= 0
        experts = jnp.where(kept, ids, -1).astype(F32)
        own_slots = (slots - lax.axis_index("ep") * cap).astype(F32)
        gap = ((0, 0), (0, GATE_ROW - top_k), (0, 0))
        meta = jnp.concatenate([jnp.pad(a, gap) for a in (experts, gates, own_slots)], axis=1)

        dims = (micro, seq, model, heads, head_dim, local_experts, cap, top_k, ff, stages)
        hbm = pl.BlockSpec(memory_space=pl.ANY)
        vmem = pl.BlockSpec(memory_space=pltpu.VMEM)
        dma = pltpu.SemaphoreType.DMA
        pieces = seq // 32
        out, _ = pl.pallas_call(
            functools.partial(boundary_kernel, dims),
            out_shape=(jax.ShapeDtypeStruct((micro, seq, model), BF16), jax.ShapeDtypeStruct((3, heads, model, head_dim), BF16)),
            in_specs=[vmem, hbm, hbm, vmem, vmem] + [hbm] * 7,
            out_specs=(hbm, hbm),
            scratch_shapes=[
                pltpu.VMEM((3, micro, META_ROWS, seq), F32),
                pltpu.VMEM((4, micro, seq, META_ROWS), F32),
                pltpu.VMEM((micro, seq, model), F32),
                pltpu.VMEM((micro, seq, model), F32),
                pltpu.VMEM((micro, seq, model), F32),
                pltpu.VMEM((micro, seq, model), F32),
                pltpu.VMEM((micro, seq, model), F32),
                pltpu.VMEM((micro, seq, model), F32),
                pltpu.VMEM((micro, seq, model), BF16),
                pltpu.VMEM((micro, seq, model), BF16),
                dma((3,)), dma((3,)),
                dma((micro, 2)), dma((micro, 2)),
                dma((micro, 2)), dma((micro, 2)),
                dma((micro, pieces)), dma((micro, pieces)),
                dma((micro, pieces)), dma((micro, pieces)),
                dma((2, 2)), dma((5,)), dma((WSLOTS, 3)), dma((OSLOTS,)), dma((RIN,)), dma((ROUT,)),
            ],
            compiler_params=pltpu.CompilerParams(collective_id=0, has_side_effects=True, vmem_limit_bytes=67043328),
        )(
            meta,
            expert_out[0],
            residual[0, :, 0],
            norm_moe, norm_attn,
            w_gate[0], w_up[0], w_down[0],
            w_query[0], w_key[0], w_value[0],
            w_out[0].reshape(heads * head_dim, model),
        )
        return out[None, :, None]

    in_specs = (tok_spec,) * 5 + (vec_spec, mat_spec, mat_spec, mat_spec, vec_spec, head_spec, head_spec, head_spec, head_spec)
    return jax.shard_map(device_step, mesh=mesh, in_specs=in_specs, out_specs=tok_spec, check_vma=False)
```

```python
import functools

import jax
import jax.numpy as jnp
from jax import lax
from jax.experimental import pallas as pl
from jax.experimental.pallas import tpu as pltpu
from jax.sharding import PartitionSpec as P

EPSILON = 1e-6
MESH = pl.DeviceIdType.MESH
F32, BF16 = jnp.float32, jnp.bfloat16
BF16_MAX = 3.3895313892515355e38
META_ROWS = 48
GATE_ROW = 16
SLOT_ROW = 32
RIN, ROUT, D_BLK, WSLOTS, OROWS = 6, 4, 64, 4, 1024


def boundary_kernel(dims, meta, rows_hbm, resid_hbm, norm_moe, norm_attn, wg_hbm, wu_hbm, wd_hbm, wq_hbm, wk_hbm, wv_hbm, wo_hbm,
                    out_hbm, wrel_hbm,
                    meta_all, meta_cols, send_part, recv_part, mine, y_recv, recv_own, acc, y_send, y_in,
                    meta_ss, meta_rs, part_ss, part_rs, own_ss, own_rs, y_ss, y_rs, z_ss, z_rs, row_sem, misc_sem, w_sem, o_sem, rl_in, rl_out):
    micro, seq, model, heads, head_dim, local_experts, cap, top_k, ff, stages = dims
    local_cols = local_experts * cap
    half = seq // 2
    piece = 32
    pieces = seq // piece
    per_half = half // piece

    me = lax.axis_index("ep")
    stage = lax.axis_index("pp")
    chip, core = me // 2, me % 2
    partner = chip * 2 + (1 - core)
    across = (1 - chip) * 2 + core
    diag = (1 - chip) * 2 + (1 - core)
    nxt, prv = (stage + 1) % stages, (stage + stages - 1) % stages

    barrier = pltpu.get_barrier_semaphore()
    for peer in (partner, across, diag):
        pl.semaphore_signal(barrier, inc=1, device_id={"ep": peer}, device_id_type=MESH)
    for peer in (nxt, prv):
        pl.semaphore_signal(barrier, inc=1, device_id={"pp": peer}, device_id_type=MESH)
    pl.semaphore_wait(barrier, 5)

    def meta_copy(rel, peer):
        return pltpu.make_async_remote_copy(src_ref=meta, dst_ref=meta_all.at[rel - 1], send_sem=meta_ss.at[rel - 1], recv_sem=meta_rs.at[rel - 1], device_id={"ep": peer}, device_id_type=MESH)

    def part_copy(m, c):
        sl = pl.ds(pl.multiple_of(c * half, half), half)
        return pltpu.make_async_remote_copy(src_ref=send_part.at[m, sl], dst_ref=recv_part.at[m, sl], send_sem=part_ss.at[m, c], recv_sem=part_rs.at[m, c], device_id={"ep": partner}, device_id_type=MESH)

    def own_copy(m, c):
        sl = pl.ds(pl.multiple_of(c * half, half), half)
        return pltpu.make_async_remote_copy(src_ref=send_part.at[m, sl], dst_ref=recv_own.at[m, sl], send_sem=own_ss.at[m, c], recv_sem=own_rs.at[m, c], device_id={"ep": partner}, device_id_type=MESH)

    def y_copy(m, k):
        sl = pl.ds(pl.multiple_of(k * piece, piece), piece)
        return pltpu.make_async_remote_copy(src_ref=mine.at[m, sl], dst_ref=y_recv.at[m, sl], send_sem=y_ss.at[m, k], recv_sem=y_rs.at[m, k], device_id={"ep": across}, device_id_type=MESH)

    def z_copy(m, k):
        sl = pl.ds(pl.multiple_of(k * piece, piece), piece)
        return pltpu.make_async_remote_copy(src_ref=y_send.at[m, sl], dst_ref=y_in.at[m, sl], send_sem=z_ss.at[m, k], recv_sem=z_rs.at[m, k], device_id={"pp": nxt}, device_id_type=MESH)

    for rel, peer in ((2, across), (3, diag), (1, partner)):
        meta_copy(rel, peer).start()

    def finish(m, lo, hi):
        def body(k, carry):
            sl = pl.ds(pl.multiple_of(k * piece, piece), piece)
            y_copy(m, k).wait()
            y_send[m, sl] = (acc[m, sl] + y_recv[m, sl]).astype(BF16)
            z_copy(m, k).start()
            return carry

        lax.fori_loop(lo, hi, body, 0)

    def phase_one(rbuf, wbuf, wg, wu, wd, xs, hid, resid, spread, pick, rin, rout):
        def rows_copy(p, ab):
            m = p % 2
            far = 1 - p // 2
            owner_a = far * diag + (1 - far) * partner
            owner_b = far * across + (1 - far) * me
            owner = owner_a if ab == 0 else owner_b
            src = rows_hbm.at[m, :, pl.ds(pl.multiple_of(owner * cap, cap), cap), :]
            at = (2 * p + ab) % 3
            return pltpu.make_async_copy(src, rbuf.at[at], row_sem.at[at])

        rows_copy(0, 0).start()
        rows_copy(0, 1).start()
        res_cp = pltpu.make_async_copy(resid_hbm, resid, misc_sem.at[0])
        wg_cp = pltpu.make_async_copy(wg_hbm, wg, misc_sem.at[1])
        wu_cp = pltpu.make_async_copy(wu_hbm, wu, misc_sem.at[2])
        wd_cp = pltpu.make_async_copy(wd_hbm, wd, misc_sem.at[3])
        for cp in (res_cp, wg_cp, wu_cp, wd_cp):
            cp.start()

        for m in range(micro):
            meta_cols[0, m] = meta[m].T
        for rel, peer in ((2, across), (3, diag), (1, partner)):
            meta_copy(rel, peer).wait()
            for m in range(micro):
                meta_cols[rel, m] = meta_all[rel - 1, m].T

        group = 32
        lane = (lax.broadcasted_iota(jnp.int32, (group, local_experts), 1) + local_experts * me).astype(F32)
        lane_slot = (lax.broadcasted_iota(jnp.int32, (group, 256), 1) % cap).astype(F32)
        from_row = lax.broadcasted_iota(jnp.int32, (local_experts, 256), 0)
        to_col = lax.broadcasted_iota(jnp.int32, (local_experts, 256), 1) // cap
        for kb in range(local_cols // 256):
            spread[kb] = jnp.where(from_row == to_col + kb * (256 // cap), 1.0, 0.0).astype(BF16)

        sub = 256 // heads
        mat_blocks = model // D_BLK
        row = lax.broadcasted_iota(jnp.int32, (256, 256), 0)
        col = lax.broadcasted_iota(jnp.int32, (256, 256), 1)
        pick[...] = jnp.where(col == (row % sub) * heads + row // sub, 1.0, 0.0).astype(BF16)

        def in_copy(src, b):
            at = pl.ds(pl.multiple_of(b % mat_blocks * D_BLK, D_BLK), D_BLK)
            return pltpu.make_async_copy(src.at[at], rin.at[b % RIN], rl_in.at[b % RIN])

        def in_start(b):
            for mat, src in enumerate((wq_hbm, wk_hbm, wv_hbm)):
                pl.when(b // mat_blocks == mat)(lambda: in_copy(src, b).start())

        def out_copy(b):
            at = pl.ds(pl.multiple_of(b % mat_blocks * D_BLK, D_BLK), D_BLK)
            return pltpu.make_async_copy(rout.at[b % ROUT], wrel_hbm.at[b // mat_blocks, :, at, :], rl_out.at[b % ROUT])

        for b in range(RIN - 2):
            in_copy(wq_hbm, b).start()

        def partial_sum(p, c, ab, dst, ride=False):
            m = p % 2
            far = 1 - p // 2
            rel = (1 + 2 * far) if ab == 0 else 2 * far
            tok = pl.ds(pl.multiple_of(c * half, half), half)
            table = meta_cols[rel, m, tok, :]

            for r in range(half // group):
                rows = slice(r * group, (r + 1) * group)
                gate = jnp.zeros((group, local_experts), F32)
                slot = jnp.zeros((group, local_experts), F32)
                for j in range(top_k):
                    hit = table[rows, j:j + 1] == lane
                    gate = jnp.where(hit, table[rows, GATE_ROW + j:GATE_ROW + j + 1], gate)
                    slot = jnp.where(hit, table[rows, SLOT_ROW + j:SLOT_ROW + j + 1], slot)
                hi = jnp.minimum(gate, BF16_MAX).astype(BF16)
                rest = gate - hi.astype(F32)
                mid = rest.astype(BF16)
                low = (rest - mid.astype(F32)).astype(BF16)
                packed = jnp.concatenate([slot.astype(BF16), hi, mid, low], axis=0)
                for kb in range(local_cols // 256):
                    wide = jnp.dot(packed, spread[kb], preferred_element_type=F32)
                    keep = wide[0:group] == lane_slot
                    for part in range(3):
                        term = jnp.where(keep, wide[(part + 1) * group:(part + 2) * group], 0.0)
                        wbuf[ab, part * half + r * group:part * half + (r + 1) * group, kb * 256:(kb + 1) * 256] = term.astype(BF16)

            def mul(n, carry):
                nn = pl.ds(pl.multiple_of(n * 512, 512), 512)
                b0 = 2 * (((2 * p + c - 2) * 2 + ab) * (model // 512) + n)
                if ride:
                    for b in (b0, b0 + 1):
                        in_copy(wq_hbm, b).wait()
                        in_start(b + RIN - 2)

                        @pl.when(b >= ROUT)
                        def _():
                            out_copy(b - ROUT).wait()
                rr = rbuf[(2 * p + ab) % 3, :, :, nn].reshape(local_cols, 512)
                d = jnp.dot(wbuf[ab], rr, preferred_element_type=F32)
                dst[m, tok, nn] = d[0:half] + d[half:2 * half] + d[2 * half:3 * half]
                if ride:
                    for b in (b0, b0 + 1):
                        for i in range(D_BLK // sub):
                            tile = rin[b % RIN, i * sub:(i + 1) * sub].reshape(sub * heads, head_dim)
                            moved = jnp.dot(pick[...], tile, preferred_element_type=F32).astype(BF16)
                            rout[b % ROUT, :, i * sub:(i + 1) * sub, :] = moved.reshape(heads, sub, head_dim)
                        out_copy(b).start()
                return carry

            lax.fori_loop(0, model // 512, mul, 0)

        def pair_step(q, ride):
            p, c = q // 2, q % 2
            m = p % 2

            @pl.when(c == 0)
            def _():
                rows_copy(p, 0).wait()
                rows_copy(p, 1).wait()
                pl.when(p < 3)(lambda: rows_copy(p + 1, 0).start())

            pl.when(p >= 2)(lambda: part_copy(m, c).wait_send())
            partial_sum(p, c, 0, send_part, ride)
            pl.when((p < 3) & (c == 1))(lambda: rows_copy(p + 1, 1).start())
            pl.when(p < 2)(lambda: part_copy(m, c).start())
            pl.when(p >= 2)(lambda: own_copy(m, c).start())

            @pl.when(p < 2)
            def _():
                partial_sum(p, c, 1, mine, ride)
                part_copy(m, c).wait_recv()

                def add(k, carry):
                    sl = pl.ds(pl.multiple_of(k * piece, piece), piece)
                    mine[m, sl] = mine[m, sl] + recv_part[m, sl]
                    y_copy(m, k).start()
                    return carry

                lax.fori_loop(c * per_half, (c + 1) * per_half, add, 0)

            if ride:
                pl.when(p >= 2)(lambda: partial_sum(p, c, 1, acc, ride))

        def shared(m):
            def norm(k, carry):
                sl = pl.ds(pl.multiple_of(k * piece, piece), piece)
                v = resid[m, sl].astype(F32)
                inv = lax.rsqrt(jnp.mean(v * v, axis=-1, keepdims=True) + EPSILON)
                xs[sl] = (v * inv * norm_moe[...]).astype(BF16)
                return carry

            lax.fori_loop(0, pieces, norm, 0)

            def up(n, carry):
                nn = pl.ds(pl.multiple_of(n * 256, 256), 256)
                g = jnp.dot(xs[...], wg[:, nn], preferred_element_type=F32)
                u = jnp.dot(xs[...], wu[:, nn], preferred_element_type=F32)
                hid[:, nn] = (g * (1.0 / (1.0 + jnp.exp(-g))) * u).astype(BF16)
                return carry

            lax.fori_loop(0, ff // 256, up, 0)
            for c in range(2):
                own_copy(m, c).wait()

            def down(n, carry):
                nn = pl.ds(pl.multiple_of(n * 256, 256), 256)
                s = jnp.dot(hid[...], wd[:, nn], preferred_element_type=F32).astype(BF16)
                acc[m, :, nn] = (resid[m, :, nn].astype(F32) + s.astype(F32)) + (acc[m, :, nn] + recv_own[m, :, nn])
                return carry

            lax.fori_loop(0, model // 256, down, 0)

        def stage_step(t, carry):
            def riding(c, inner):
                pair_step(2 * t + c, True)
                return inner

            lax.fori_loop(0, 2, riding, 0)

            @pl.when(t >= 2)
            def _():
                @pl.when(t == 2)
                def _():
                    for cp in (res_cp, wg_cp, wu_cp, wd_cp):
                        cp.wait()
                shared(t - 2)

                @pl.when(t == 2)
                def _():
                    finish(0, 0, 6)
            return carry

        def first(q, carry):
            pair_step(q, False)
            return carry

        lax.fori_loop(0, 2, first, 0)
        lax.fori_loop(1, 4, stage_step, 0)
        for b in range(3 * mat_blocks - ROUT, 3 * mat_blocks):
            out_copy(b).wait()

    pl.run_scoped(
        phase_one,
        pltpu.VMEM((3, local_experts, cap, model), BF16),
        pltpu.VMEM((2, 3 * half, local_cols), BF16),
        pltpu.VMEM((model, ff), BF16),
        pltpu.VMEM((model, ff), BF16),
        pltpu.VMEM((ff, model), BF16),
        pltpu.VMEM((seq, model), BF16),
        pltpu.VMEM((seq, ff), BF16),
        pltpu.VMEM((micro, seq, model), BF16),
        pltpu.VMEM((local_cols // 256, local_experts, 256), BF16),
        pltpu.VMEM((256, 256), BF16),
        pltpu.VMEM((RIN, D_BLK, heads, head_dim), BF16),
        pltpu.VMEM((ROUT, heads, D_BLK, head_dim), BF16),
    )

    def phase_two(wbuf, obuf, wob, xbuf, mixed):
        def w_copy(h, mat):
            return pltpu.make_async_copy(wrel_hbm.at[mat, h], wbuf.at[h % WSLOTS, mat], w_sem.at[h % WSLOTS, mat])

        n_out = heads * head_dim // OROWS

        def o_copy(n):
            return pltpu.make_async_copy(wo_hbm.at[pl.ds(pl.multiple_of(n * OROWS, OROWS), OROWS)], wob.at[n % 2], o_sem.at[n % 2])

        for h in range(WSLOTS - 1):
            for mat in range(3):
                w_copy(h, mat).start()
        o_copy(0).start()

        qi = lax.broadcasted_iota(jnp.int32, (seq, seq), 0)
        ki = lax.broadcasted_iota(jnp.int32, (seq, seq), 1)
        causal = qi >= ki
        scale = 1.0 / (head_dim ** 0.5)

        def attention(m):
            last = m == micro - 1

            def norm(k, carry):
                sl = pl.ds(pl.multiple_of(k * piece, piece), piece)
                z_copy(m, k).wait()
                v = y_in[m, sl].astype(F32)
                inv = lax.rsqrt(jnp.mean(v * v, axis=-1, keepdims=True) + EPSILON)
                xbuf[sl] = (v * inv * norm_attn[...]).astype(BF16)
                return carry

            lax.fori_loop(0, pieces, norm, 0)

            def head(h, carry):
                slot = h % WSLOTS
                for mat in range(3):
                    w_copy(h, mat).wait()

                def prefetch():
                    for mat in range(3):
                        w_copy((h + WSLOTS - 1) % heads, mat).start()

                if last:
                    pl.when(h + WSLOTS - 1 < heads)(prefetch)
                else:
                    prefetch()
                x = xbuf[...]
                q = jnp.dot(x, wbuf[slot, 0], preferred_element_type=F32).astype(BF16)
                k = jnp.dot(x, wbuf[slot, 1], preferred_element_type=F32).astype(BF16)
                v = jnp.dot(x, wbuf[slot, 2], preferred_element_type=F32).astype(BF16)
                s = lax.dot_general(q, k, (((1,), (1,)), ((), ())), preferred_element_type=F32) * scale
                s = jnp.where(causal, s, -1e30)
                e = jnp.exp(s - jnp.max(s, axis=-1, keepdims=True))
                total = jnp.sum(e, axis=-1, keepdims=True)
                o = jnp.dot(e.astype(BF16), v, preferred_element_type=F32) / total
                mixed[:, pl.ds(pl.multiple_of(h * head_dim, head_dim), head_dim)] = o.astype(BF16)
                if not last:
                    pl.when(h % 4 == 2)(lambda: finish(1, 2 + h // 4, 3 + h // 4))
                return carry

            def proj(n, carry):
                lax.fori_loop(n * heads // n_out, (n + 1) * heads // n_out, head, 0)
                o_copy(n).wait()
                if last:
                    pl.when(n + 1 < n_out)(lambda: o_copy(n + 1).start())
                else:
                    o_copy((n + 1) % n_out).start()
                kk = pl.ds(pl.multiple_of(n * OROWS, OROWS), OROWS)
                for j in range(model // 512):
                    nn = slice(j * 512, (j + 1) * 512)
                    part = jnp.dot(mixed[:, kk], wob[n % 2, :, nn], preferred_element_type=F32)
                    acc[m, :, nn] = jnp.where(n == 0, part, acc[m, :, nn] + part)
                return carry

            lax.fori_loop(0, n_out, proj, 0)

            def residual(k, carry):
                sl = pl.ds(pl.multiple_of(k * piece, piece), piece)
                obuf[sl] = (y_in[m, sl].astype(F32) + acc[m, sl].astype(BF16).astype(F32)).astype(BF16)
                return carry

            lax.fori_loop(0, pieces, residual, 0)
            out_cp = pltpu.make_async_copy(obuf, out_hbm.at[m], misc_sem.at[4])
            out_cp.start()
            out_cp.wait()

        finish(0, 6, 8)
        finish(1, 0, 2)
        attention(0)
        finish(1, 6, 8)
        attention(1)

    pl.run_scoped(
        phase_two,
        pltpu.VMEM((WSLOTS, 3, model, head_dim), BF16),
        pltpu.VMEM((seq, model), BF16),
        pltpu.VMEM((2, OROWS, model), BF16),
        pltpu.VMEM((seq, model), BF16),
        pltpu.VMEM((seq, heads * head_dim), BF16),
    )


def solution(mesh):
    stages = mesh.shape["pp"]
    ep_size = mesh.shape["ep"]
    tok_spec = P("pp", "data", "ep", None, None)
    vec_spec = P("pp", None)
    mat_spec = P("pp", None, None)
    head_spec = P("pp", None, None, None)

    def device_step(expert_out, expert_ids, slot_ids, gate_weights, residual, norm_moe, w_gate, w_up, w_down, norm_attn, w_query, w_key, w_value, w_out):
        micro = expert_out.shape[1]
        local_experts, slots_total, model = expert_out.shape[2:]
        cap = slots_total // ep_size
        seq, top_k = expert_ids.shape[3:]
        heads, head_dim = w_query.shape[2:]
        ff = w_gate.shape[2]
        ids = jnp.swapaxes(expert_ids[0, :, 0], 1, 2)
        slots = jnp.swapaxes(slot_ids[0, :, 0], 1, 2)
        gates = jnp.swapaxes(gate_weights[0, :, 0], 1, 2)
        kept = slots >= 0
        experts = jnp.where(kept, ids, -1).astype(F32)
        own_slots = (slots - lax.axis_index("ep") * cap).astype(F32)
        gap = ((0, 0), (0, GATE_ROW - top_k), (0, 0))
        meta = jnp.concatenate([jnp.pad(a, gap) for a in (experts, gates, own_slots)], axis=1)

        dims = (micro, seq, model, heads, head_dim, local_experts, cap, top_k, ff, stages)
        hbm = pl.BlockSpec(memory_space=pl.ANY)
        vmem = pl.BlockSpec(memory_space=pltpu.VMEM)
        dma = pltpu.SemaphoreType.DMA
        pieces = seq // 32
        out, _ = pl.pallas_call(
            functools.partial(boundary_kernel, dims),
            out_shape=(jax.ShapeDtypeStruct((micro, seq, model), BF16), jax.ShapeDtypeStruct((3, heads, model, head_dim), BF16)),
            in_specs=[vmem, hbm, hbm, vmem, vmem] + [hbm] * 7,
            out_specs=(hbm, hbm),
            scratch_shapes=[
                pltpu.VMEM((3, micro, META_ROWS, seq), F32),
                pltpu.VMEM((4, micro, seq, META_ROWS), F32),
                pltpu.VMEM((micro, seq, model), F32),
                pltpu.VMEM((micro, seq, model), F32),
                pltpu.VMEM((micro, seq, model), F32),
                pltpu.VMEM((micro, seq, model), F32),
                pltpu.VMEM((micro, seq, model), F32),
                pltpu.VMEM((micro, seq, model), F32),
                pltpu.VMEM((micro, seq, model), BF16),
                pltpu.VMEM((micro, seq, model), BF16),
                dma((3,)), dma((3,)),
                dma((micro, 2)), dma((micro, 2)),
                dma((micro, 2)), dma((micro, 2)),
                dma((micro, pieces)), dma((micro, pieces)),
                dma((micro, pieces)), dma((micro, pieces)),
                dma((3,)), dma((5,)), dma((WSLOTS, 3)), dma((2,)), dma((RIN,)), dma((ROUT,)),
            ],
            compiler_params=pltpu.CompilerParams(collective_id=0, has_side_effects=True, vmem_limit_bytes=67043328),
        )(
            meta,
            expert_out[0],
            residual[0, :, 0],
            norm_moe, norm_attn,
            w_gate[0], w_up[0], w_down[0],
            w_query[0], w_key[0], w_value[0],
            w_out[0].reshape(heads * head_dim, model),
        )
        return out[None, :, None]

    in_specs = (tok_spec,) * 5 + (vec_spec, mat_spec, mat_spec, mat_spec, vec_spec, head_spec, head_spec, head_spec, head_spec)
    return jax.shard_map(device_step, mesh=mesh, in_specs=in_specs, out_specs=tok_spec, check_vma=False)
```

```python
import functools

import jax
import jax.numpy as jnp
from jax import lax
from jax.experimental import pallas as pl
from jax.experimental.pallas import tpu as pltpu
from jax.sharding import PartitionSpec as P

EPSILON = 1e-6
MESH = pl.DeviceIdType.MESH
F32, BF16 = jnp.float32, jnp.bfloat16
BF16_MAX = 3.3895313892515355e38
META_ROWS = 48
GATE_ROW = 16
SLOT_ROW = 32
RIN, ROUT, D_BLK, WSLOTS, OROWS = 6, 4, 64, 4, 1024


def boundary_kernel(dims, meta, rows_hbm, resid_hbm, norm_moe, norm_attn, wg_hbm, wu_hbm, wd_hbm, wq_hbm, wk_hbm, wv_hbm, wo_hbm,
                    out_hbm, wrel_hbm,
                    meta_all, send_part, recv_part, mine, y_recv, recv_own, acc, y_send, y_in,
                    meta_ss, meta_rs, part_ss, part_rs, own_ss, own_rs, y_ss, y_rs, z_ss, z_rs, row_sem, misc_sem, w_sem, o_sem, rl_in, rl_out):
    micro, seq, model, heads, head_dim, local_experts, cap, top_k, ff, stages = dims
    local_cols = local_experts * cap
    half = seq // 2
    piece = 32
    pieces = seq // piece
    per_half = half // piece

    me = lax.axis_index("ep")
    stage = lax.axis_index("pp")
    chip, core = me // 2, me % 2
    partner = chip * 2 + (1 - core)
    across = (1 - chip) * 2 + core
    diag = (1 - chip) * 2 + (1 - core)
    nxt, prv = (stage + 1) % stages, (stage + stages - 1) % stages

    def meta_copy(rel, peer):
        return pltpu.make_async_remote_copy(src_ref=meta, dst_ref=meta_all.at[rel], send_sem=meta_ss.at[rel - 1], recv_sem=meta_rs.at[rel - 1], device_id={"ep": peer}, device_id_type=MESH)

    def part_copy(m, c):
        sl = pl.ds(pl.multiple_of(c * half, half), half)
        return pltpu.make_async_remote_copy(src_ref=send_part.at[m, sl], dst_ref=recv_part.at[m, sl], send_sem=part_ss.at[m, c], recv_sem=part_rs.at[m, c], device_id={"ep": partner}, device_id_type=MESH)

    def own_copy(m, c):
        sl = pl.ds(pl.multiple_of(c * half, half), half)
        return pltpu.make_async_remote_copy(src_ref=send_part.at[m, sl], dst_ref=recv_own.at[m, sl], send_sem=own_ss.at[m, c], recv_sem=own_rs.at[m, c], device_id={"ep": partner}, device_id_type=MESH)

    def y_copy(m, k):
        sl = pl.ds(pl.multiple_of(k * piece, piece), piece)
        return pltpu.make_async_remote_copy(src_ref=mine.at[m, sl], dst_ref=y_recv.at[m, sl], send_sem=y_ss.at[m, k], recv_sem=y_rs.at[m, k], device_id={"ep": across}, device_id_type=MESH)

    def z_copy(m, k):
        sl = pl.ds(pl.multiple_of(k * piece, piece), piece)
        return pltpu.make_async_remote_copy(src_ref=y_send.at[m, sl], dst_ref=y_in.at[m, sl], send_sem=z_ss.at[m, k], recv_sem=z_rs.at[m, k], device_id={"pp": nxt}, device_id_type=MESH)

    def finish(m, lo, hi):
        def body(k, carry):
            sl = pl.ds(pl.multiple_of(k * piece, piece), piece)
            y_copy(m, k).wait()
            y_send[m, sl] = (acc[m, sl] + recv_own[m, sl] + y_recv[m, sl]).astype(BF16)
            z_copy(m, k).start()
            return carry

        lax.fori_loop(lo, hi, body, 0)

    def phase_one(rbuf, wbuf, wg, wu, wd, xs, hid, resid, spread, packed, pick, rin, rout):
        def rows_copy(p, ab):
            m = p % 2
            far = 1 - p // 2
            owner_a = far * diag + (1 - far) * partner
            owner_b = far * across + (1 - far) * me
            owner = owner_a if ab == 0 else owner_b
            src = rows_hbm.at[m, :, pl.ds(pl.multiple_of(owner * cap, cap), cap), :]
            at = (2 * p + ab) % 3
            return pltpu.make_async_copy(src, rbuf.at[at], row_sem.at[at])

        rows_copy(0, 0).start()
        rows_copy(0, 1).start()
        res_cp = pltpu.make_async_copy(resid_hbm, resid, misc_sem.at[0])
        wg_cp = pltpu.make_async_copy(wg_hbm, wg, misc_sem.at[1])
        wu_cp = pltpu.make_async_copy(wu_hbm, wu, misc_sem.at[2])
        wd_cp = pltpu.make_async_copy(wd_hbm, wd, misc_sem.at[3])
        for cp in (res_cp, wg_cp, wu_cp, wd_cp):
            cp.start()

        barrier = pltpu.get_barrier_semaphore()
        for peer in (partner, across, diag):
            pl.semaphore_signal(barrier, inc=1, device_id={"ep": peer}, device_id_type=MESH)
        for peer in (nxt, prv):
            pl.semaphore_signal(barrier, inc=1, device_id={"pp": peer}, device_id_type=MESH)
        pl.semaphore_wait(barrier, 5)

        for rel, peer in ((2, across), (3, diag), (1, partner)):
            meta_copy(rel, peer).start()

        for cp in (res_cp, wg_cp, wu_cp, wd_cp):
            cp.wait()

        def shared(m, carry):
            def norm(k, carry):
                sl = pl.ds(pl.multiple_of(k * piece, piece), piece)
                v = resid[m, sl].astype(F32)
                inv = lax.rsqrt(jnp.mean(v * v, axis=-1, keepdims=True) + EPSILON)
                xs[sl] = (v * inv * norm_moe[...]).astype(BF16)
                return carry

            lax.fori_loop(0, pieces, norm, 0)

            def up(n, carry):
                nn = pl.ds(pl.multiple_of(n * 256, 256), 256)
                g = jnp.dot(xs[...], wg[:, nn], preferred_element_type=F32)
                u = jnp.dot(xs[...], wu[:, nn], preferred_element_type=F32)
                hid[:, nn] = (g * (1.0 / (1.0 + jnp.exp(-g))) * u).astype(BF16)
                return carry

            lax.fori_loop(0, ff // 256, up, 0)
            def down(n, carry):
                nn = pl.ds(pl.multiple_of(n * 256, 256), 256)
                s = jnp.dot(hid[...], wd[:, nn], preferred_element_type=F32).astype(BF16)
                acc[m, :, nn] = resid[m, :, nn].astype(F32) + s.astype(F32)
                return carry

            lax.fori_loop(0, model // 256, down, 0)
            return carry

        lax.fori_loop(0, micro, shared, 0)

        meta_all[0] = meta[...]
        for rel, peer in ((2, across), (3, diag), (1, partner)):
            meta_copy(rel, peer).wait()

        group = 32
        expert = (lax.broadcasted_iota(jnp.int32, (local_experts, half), 0) + local_experts * me).astype(F32)
        lane_slot = (lax.broadcasted_iota(jnp.int32, (group, 256), 1) % cap).astype(F32)
        from_row = lax.broadcasted_iota(jnp.int32, (local_experts, 256), 0)
        to_col = lax.broadcasted_iota(jnp.int32, (local_experts, 256), 1) // cap
        for kb in range(local_cols // 256):
            spread[kb] = jnp.where(from_row == to_col + kb * (256 // cap), 1.0, 0.0).astype(BF16)

        sub = 256 // heads
        mat_blocks = model // D_BLK
        row = lax.broadcasted_iota(jnp.int32, (256, 256), 0)
        col = lax.broadcasted_iota(jnp.int32, (256, 256), 1)
        pick[...] = jnp.where(col == (row % sub) * heads + row // sub, 1.0, 0.0).astype(BF16)

        def in_copy(src, b):
            at = pl.ds(pl.multiple_of(b % mat_blocks * D_BLK, D_BLK), D_BLK)
            return pltpu.make_async_copy(src.at[at], rin.at[b % RIN], rl_in.at[b % RIN])

        def in_start(b):
            for mat, src in enumerate((wq_hbm, wk_hbm, wv_hbm)):
                pl.when(b // mat_blocks == mat)(lambda: in_copy(src, b).start())

        def out_copy(b):
            at = pl.ds(pl.multiple_of(b % mat_blocks * D_BLK, D_BLK), D_BLK)
            return pltpu.make_async_copy(rout.at[b % ROUT], wrel_hbm.at[b // mat_blocks, :, at, :], rl_out.at[b % ROUT])

        for b in range(RIN - 2):
            in_copy(wq_hbm, b).start()

        def gate_table(u):
            u = jnp.minimum(u, 15)
            p, c, ab = u // 4, (u // 2) % 2, u % 2
            rel = (1 - ab) + 2 * (1 - p // 2)
            tab = meta_all[rel, p % 2, :, pl.ds(pl.multiple_of(c * half, half), half)]
            gates, slots = [], []
            for r in range(local_experts // 32):
                ids = expert[r * 32:(r + 1) * 32]
                gate = jnp.zeros((32, half), F32)
                slot = jnp.zeros((32, half), F32)
                for j in range(top_k):
                    hit = tab[j:j + 1] == ids
                    gate = jnp.where(hit, tab[GATE_ROW + j:GATE_ROW + j + 1], gate)
                    slot = jnp.where(hit, tab[SLOT_ROW + j:SLOT_ROW + j + 1], slot)
                gates.append(gate)
                slots.append(slot)
            gate = jnp.concatenate(gates, axis=0).T
            slot = jnp.concatenate(slots, axis=0).T
            hi = jnp.minimum(gate, BF16_MAX).astype(BF16)
            rest = gate - hi.astype(F32)
            mid = rest.astype(BF16)
            low = (rest - mid.astype(F32)).astype(BF16)
            for part, value in enumerate((slot.astype(BF16), hi, mid, low)):
                packed[:, part] = value.reshape(half // group, group, local_experts)

        def spread_group(to, r):
            mix = packed[r].reshape(4 * group, local_experts)
            for kb in range(local_cols // 256):
                wide = jnp.dot(mix, spread[kb], preferred_element_type=F32)
                keep = wide[0:group] == lane_slot
                for part in range(3):
                    term = jnp.where(keep, wide[(part + 1) * group:(part + 2) * group], 0.0)
                    at = pl.ds(pl.multiple_of(part * half + r * group, group), group)
                    wbuf[to, at, kb * 256:(kb + 1) * 256] = term.astype(BF16)

        def first_spread(r, carry):
            spread_group(0, r)
            return carry

        gate_table(0)
        lax.fori_loop(0, half // group, first_spread, 0)
        gate_table(1)

        def partial_sum(p, c, ab, dst, ride=False):
            m = p % 2
            tok = pl.ds(pl.multiple_of(c * half, half), half)

            def mul(n, carry):
                b0 = 2 * (((2 * p + c - 2) * 2 + ab) * (model // 512) + n)
                if ride:
                    for b in (b0, b0 + 1):
                        in_copy(wq_hbm, b).wait()
                        in_start(b + RIN - 2)
                        pl.when(b >= ROUT)(lambda: out_copy(b - ROUT).wait())
                for part in range(2):
                    nn = pl.ds(pl.multiple_of(n * 512 + part * 256, 256), 256)
                    rr = rbuf[(2 * p + ab) % 3, :, :, nn].reshape(local_cols, 256)
                    d = jnp.dot(wbuf[ab], rr, preferred_element_type=F32)
                    d = d[0:half] + d[half:2 * half] + d[2 * half:3 * half]
                    dst[m, tok, nn] = dst[m, tok, nn] + d if dst is acc else d
                    if ride:
                        b = b0 + part
                        for i in range(D_BLK // sub):
                            tile = rin[b % RIN, i * sub:(i + 1) * sub].reshape(sub * heads, head_dim)
                            moved = jnp.dot(pick[...], tile, preferred_element_type=F32).astype(BF16)
                            rout[b % ROUT, :, i * sub:(i + 1) * sub, :] = moved.reshape(heads, sub, head_dim)
                spread_group(1 - ab, n)
                if ride:
                    out_copy(b0).start()
                    out_copy(b0 + 1).start()
                return carry

            lax.fori_loop(0, model // 512, mul, 0)
            gate_table(2 * (2 * p + c) + ab + 2)

        def pair_step(q, ride):
            p, c = q // 2, q % 2
            m = p % 2

            @pl.when(c == 0)
            def _():
                rows_copy(p, 0).wait()
                rows_copy(p, 1).wait()
                pl.when(p < 3)(lambda: rows_copy(p + 1, 0).start())

            pl.when(p >= 2)(lambda: part_copy(m, c).wait_send())
            partial_sum(p, c, 0, send_part, ride)
            pl.when((p < 3) & (c == 1))(lambda: rows_copy(p + 1, 1).start())
            pl.when(p < 2)(lambda: part_copy(m, c).start())
            pl.when(p >= 2)(lambda: own_copy(m, c).start())

            @pl.when(p < 2)
            def _():
                partial_sum(p, c, 1, mine, ride)
                part_copy(m, c).wait_recv()

                def add(k, carry):
                    sl = pl.ds(pl.multiple_of(k * piece, piece), piece)
                    mine[m, sl] = mine[m, sl] + recv_part[m, sl]
                    y_copy(m, k).start()
                    return carry

                lax.fori_loop(c * per_half, (c + 1) * per_half, add, 0)

            if ride:
                pl.when(p >= 2)(lambda: partial_sum(p, c, 1, acc, ride))

        def stage_step(t, carry):
            def riding(c, inner):
                pair_step(2 * t + c, True)
                return inner

            lax.fori_loop(0, 2, riding, 0)

            @pl.when(t >= 2)
            def _():
                for c in range(2):
                    own_copy(t - 2, c).wait()
                pl.when(t == 2)(lambda: finish(0, 0, 6))
            return carry

        def first(q, carry):
            pair_step(q, False)
            return carry

        lax.fori_loop(0, 2, first, 0)
        lax.fori_loop(1, 4, stage_step, 0)
        for b in range(3 * mat_blocks - ROUT, 3 * mat_blocks):
            out_copy(b).wait()

    pl.run_scoped(
        phase_one,
        pltpu.VMEM((3, local_experts, cap, model), BF16),
        pltpu.VMEM((2, 3 * half, local_cols), BF16),
        pltpu.VMEM((model, ff), BF16),
        pltpu.VMEM((model, ff), BF16),
        pltpu.VMEM((ff, model), BF16),
        pltpu.VMEM((seq, model), BF16),
        pltpu.VMEM((seq, ff), BF16),
        pltpu.VMEM((micro, seq, model), BF16),
        pltpu.VMEM((local_cols // 256, local_experts, 256), BF16),
        pltpu.VMEM((4, 4, seq // 8, local_experts), BF16),
        pltpu.VMEM((256, 256), BF16),
        pltpu.VMEM((RIN, D_BLK, heads, head_dim), BF16),
        pltpu.VMEM((ROUT, heads, D_BLK, head_dim), BF16),
    )

    def phase_two(wbuf, obuf, wob, xbuf, mixed, qkv):
        def w_copy(h, mat):
            return pltpu.make_async_copy(wrel_hbm.at[mat, h], wbuf.at[h % WSLOTS, mat], w_sem.at[h % WSLOTS, mat])

        n_out = heads * head_dim // OROWS

        def o_copy(n):
            return pltpu.make_async_copy(wo_hbm.at[pl.ds(pl.multiple_of(n * OROWS, OROWS), OROWS)], wob.at[n % 2], o_sem.at[n % 2])

        for h in range(WSLOTS - 1):
            for mat in range(3):
                w_copy(h, mat).start()
        o_copy(0).start()

        qi = lax.broadcasted_iota(jnp.int32, (seq, seq), 0)
        ki = lax.broadcasted_iota(jnp.int32, (seq, seq), 1)
        causal = qi >= ki
        scale = 1.0 / (head_dim ** 0.5)

        def attention(m):
            last = m == micro - 1

            def norm(k, carry):
                sl = pl.ds(pl.multiple_of(k * piece, piece), piece)
                z_copy(m, k).wait()
                v = y_in[m, sl].astype(F32)
                inv = lax.rsqrt(jnp.mean(v * v, axis=-1, keepdims=True) + EPSILON)
                xbuf[sl] = (v * inv * norm_attn[...]).astype(BF16)
                return carry

            lax.fori_loop(0, pieces, norm, 0)

            def softmax_head(h, between):
                s = lax.dot_general(qkv[0], qkv[1], (((1,), (1,)), ((), ())), preferred_element_type=F32) * scale
                value = qkv[2]
                between()
                s = jnp.where(causal, s, -1e30)
                e = jnp.exp(s - jnp.max(s, axis=-1, keepdims=True))
                total = jnp.sum(e, axis=-1, keepdims=True)
                between()
                o = jnp.dot(e.astype(BF16), value, preferred_element_type=F32) / total
                between()
                mixed[:, pl.ds(pl.multiple_of(h * head_dim, head_dim), head_dim)] = o.astype(BF16)

            def head(h, carry):
                slot = h % WSLOTS
                for mat in range(3):
                    w_copy(h, mat).wait()

                def prefetch():
                    for mat in range(3):
                        w_copy((h + WSLOTS - 1) % heads, mat).start()

                if last:
                    pl.when(h + WSLOTS - 1 < heads)(prefetch)
                else:
                    prefetch()
                x = xbuf[...]
                fresh = []

                def project():
                    mat = len(fresh)
                    fresh.append(jnp.dot(x, wbuf[slot, mat], preferred_element_type=F32).astype(BF16))

                softmax_head(jnp.maximum(h - 1, 0), project)
                for mat in range(3):
                    qkv[mat] = fresh[mat]
                if not last:
                    pl.when((h % 3 == 2) & (h < 12))(lambda: finish(1, 4 + h // 3, 5 + h // 3))
                return carry

            def proj(n, carry):
                o_copy(n).wait()
                if last:
                    pl.when(n + 1 < n_out)(lambda: o_copy(n + 1).start())
                else:
                    o_copy((n + 1) % n_out).start()
                kk = pl.ds(pl.multiple_of(n * OROWS, OROWS), OROWS)
                for j in range(model // 512):
                    nn = slice(j * 512, (j + 1) * 512)
                    part = jnp.dot(mixed[:, kk], wob[n % 2, :, nn], preferred_element_type=F32)
                    acc[m, :, nn] = jnp.where(n == 0, part, acc[m, :, nn] + part)
                return carry

            lax.fori_loop(0, heads, head, 0)
            softmax_head(heads - 1, lambda: None)
            lax.fori_loop(0, n_out, proj, 0)

            def residual(k, carry):
                sl = pl.ds(pl.multiple_of(k * piece, piece), piece)
                obuf[sl] = (y_in[m, sl].astype(F32) + acc[m, sl].astype(BF16).astype(F32)).astype(BF16)
                return carry

            lax.fori_loop(0, pieces, residual, 0)
            out_cp = pltpu.make_async_copy(obuf, out_hbm.at[m], misc_sem.at[4])
            out_cp.start()
            out_cp.wait()

        qkv[...] = jnp.zeros_like(qkv)
        finish(0, 6, 8)
        finish(1, 0, 4)
        attention(0)
        attention(1)

    pl.run_scoped(
        phase_two,
        pltpu.VMEM((WSLOTS, 3, model, head_dim), BF16),
        pltpu.VMEM((seq, model), BF16),
        pltpu.VMEM((2, OROWS, model), BF16),
        pltpu.VMEM((seq, model), BF16),
        pltpu.VMEM((seq, heads * head_dim), BF16),
        pltpu.VMEM((3, seq, head_dim), BF16),
    )


def solution(mesh):
    stages = mesh.shape["pp"]
    ep_size = mesh.shape["ep"]
    tok_spec = P("pp", "data", "ep", None, None)
    vec_spec = P("pp", None)
    mat_spec = P("pp", None, None)
    head_spec = P("pp", None, None, None)

    def device_step(expert_out, expert_ids, slot_ids, gate_weights, residual, norm_moe, w_gate, w_up, w_down, norm_attn, w_query, w_key, w_value, w_out):
        micro = expert_out.shape[1]
        local_experts, slots_total, model = expert_out.shape[2:]
        cap = slots_total // ep_size
        seq, top_k = expert_ids.shape[3:]
        heads, head_dim = w_query.shape[2:]
        ff = w_gate.shape[2]
        ids = jnp.swapaxes(expert_ids[0, :, 0], 1, 2)
        slots = jnp.swapaxes(slot_ids[0, :, 0], 1, 2)
        gates = jnp.swapaxes(gate_weights[0, :, 0], 1, 2)
        kept = slots >= 0
        experts = jnp.where(kept, ids, -1).astype(F32)
        own_slots = (slots - lax.axis_index("ep") * cap).astype(F32)
        gap = ((0, 0), (0, GATE_ROW - top_k), (0, 0))
        meta = jnp.concatenate([jnp.pad(a, gap) for a in (experts, gates, own_slots)], axis=1)

        dims = (micro, seq, model, heads, head_dim, local_experts, cap, top_k, ff, stages)
        hbm = pl.BlockSpec(memory_space=pl.ANY)
        vmem = pl.BlockSpec(memory_space=pltpu.VMEM)
        dma = pltpu.SemaphoreType.DMA
        pieces = seq // 32
        out, _ = pl.pallas_call(
            functools.partial(boundary_kernel, dims),
            out_shape=(jax.ShapeDtypeStruct((micro, seq, model), BF16), jax.ShapeDtypeStruct((3, heads, model, head_dim), BF16)),
            in_specs=[vmem, hbm, hbm, vmem, vmem] + [hbm] * 7,
            out_specs=(hbm, hbm),
            scratch_shapes=[
                pltpu.VMEM((4, micro, META_ROWS, seq), F32),
                pltpu.VMEM((micro, seq, model), F32),
                pltpu.VMEM((micro, seq, model), F32),
                pltpu.VMEM((micro, seq, model), F32),
                pltpu.VMEM((micro, seq, model), F32),
                pltpu.VMEM((micro, seq, model), F32),
                pltpu.VMEM((micro, seq, model), F32),
                pltpu.VMEM((micro, seq, model), BF16),
                pltpu.VMEM((micro, seq, model), BF16),
                dma((3,)), dma((3,)),
                dma((micro, 2)), dma((micro, 2)),
                dma((micro, 2)), dma((micro, 2)),
                dma((micro, pieces)), dma((micro, pieces)),
                dma((micro, pieces)), dma((micro, pieces)),
                dma((3,)), dma((5,)), dma((WSLOTS, 3)), dma((2,)), dma((RIN,)), dma((ROUT,)),
            ],
            compiler_params=pltpu.CompilerParams(collective_id=0, has_side_effects=True, vmem_limit_bytes=67043328),
        )(
            meta,
            expert_out[0],
            residual[0, :, 0],
            norm_moe, norm_attn,
            w_gate[0], w_up[0], w_down[0],
            w_query[0], w_key[0], w_value[0],
            w_out[0].reshape(heads * head_dim, model),
        )
        return out[None, :, None]

    in_specs = (tok_spec,) * 5 + (vec_spec, mat_spec, mat_spec, mat_spec, vec_spec, head_spec, head_spec, head_spec, head_spec)
    return jax.shard_map(device_step, mesh=mesh, in_specs=in_specs, out_specs=tok_spec, check_vma=False)
```

```python
import functools

import jax
import jax.numpy as jnp
from jax import lax
from jax.experimental import pallas as pl
from jax.experimental.pallas import tpu as pltpu
from jax.sharding import PartitionSpec as P

EPSILON = 1e-6
MESH = pl.DeviceIdType.MESH
F32, BF16 = jnp.float32, jnp.bfloat16
BF16_MAX = 3.3895313892515355e38
META_ROWS = 48
GATE_ROW = 16
SLOT_ROW = 32
RIN, ROUT, RSTEP, D_BLK, WSLOTS, OSLOTS, OROWS = 8, 6, 2, 64, 6, 4, 512


def boundary_kernel(dims, meta, rows_hbm, resid_hbm, norm_moe, norm_attn, wg_hbm, wu_hbm, wd_hbm, wq_hbm, wk_hbm, wv_hbm, wo_hbm,
                    out_hbm, wrel_hbm,
                    meta_all, send_part, recv_part, mine, y_recv, recv_own, acc, y_send, y_in,
                    meta_ss, meta_rs, part_ss, part_rs, own_ss, own_rs, y_ss, y_rs, z_ss, z_rs, row_sem, misc_sem, w_sem, o_sem, rl_in, rl_out):
    micro, seq, model, heads, head_dim, local_experts, cap, top_k, ff, stages = dims
    local_cols = local_experts * cap
    half = seq // 2
    piece = 32
    pieces = seq // piece
    per_half = half // piece

    me = lax.axis_index("ep")
    stage = lax.axis_index("pp")
    chip, core = me // 2, me % 2
    partner = chip * 2 + (1 - core)
    across = (1 - chip) * 2 + core
    diag = (1 - chip) * 2 + (1 - core)
    nxt, prv = (stage + 1) % stages, (stage + stages - 1) % stages

    def meta_copy(rel, peer):
        return pltpu.make_async_remote_copy(src_ref=meta, dst_ref=meta_all.at[rel], send_sem=meta_ss.at[rel - 1], recv_sem=meta_rs.at[rel - 1], device_id={"ep": peer}, device_id_type=MESH)

    def part_copy(m, c):
        sl = pl.ds(pl.multiple_of(c * half, half), half)
        return pltpu.make_async_remote_copy(src_ref=send_part.at[m, sl], dst_ref=recv_part.at[m, sl], send_sem=part_ss.at[m, c], recv_sem=part_rs.at[m, c], device_id={"ep": partner}, device_id_type=MESH)

    def own_copy(m, c):
        sl = pl.ds(pl.multiple_of(c * half, half), half)
        return pltpu.make_async_remote_copy(src_ref=send_part.at[m, sl], dst_ref=recv_own.at[m, sl], send_sem=own_ss.at[m, c], recv_sem=own_rs.at[m, c], device_id={"ep": partner}, device_id_type=MESH)

    def y_copy(m, k):
        sl = pl.ds(pl.multiple_of(k * piece, piece), piece)
        return pltpu.make_async_remote_copy(src_ref=mine.at[m, sl], dst_ref=y_recv.at[m, sl], send_sem=y_ss.at[m, k], recv_sem=y_rs.at[m, k], device_id={"ep": across}, device_id_type=MESH)

    def z_copy(m, k):
        sl = pl.ds(pl.multiple_of(k * piece, piece), piece)
        return pltpu.make_async_remote_copy(src_ref=y_send.at[m, sl], dst_ref=y_in.at[m, sl], send_sem=z_ss.at[m, k], recv_sem=z_rs.at[m, k], device_id={"pp": nxt}, device_id_type=MESH)

    def finish(m, lo, hi):
        def body(k, carry):
            sl = pl.ds(pl.multiple_of(k * piece, piece), piece)
            y_copy(m, k).wait()
            y_send[m, sl] = (acc[m, sl] + recv_own[m, sl] + y_recv[m, sl]).astype(BF16)
            z_copy(m, k).start()
            return carry

        lax.fori_loop(lo, hi, body, 0)

    def phase_one(rbuf, wbuf, wg, wu, wd, xs, hid, resid, spread, packed, pick, rin, rout):
        def rows_copy(p, ab):
            m = p % 2
            far = 1 - p // 2
            owner_a = far * diag + (1 - far) * partner
            owner_b = far * across + (1 - far) * me
            owner = owner_a if ab == 0 else owner_b
            src = rows_hbm.at[m, :, pl.ds(pl.multiple_of(owner * cap, cap), cap), :]
            at = (2 * p + ab) % 3
            return pltpu.make_async_copy(src, rbuf.at[at], row_sem.at[at])

        rows_copy(0, 0).start()
        rows_copy(0, 1).start()
        res_cp = pltpu.make_async_copy(resid_hbm, resid, misc_sem.at[0])
        wg_cp = pltpu.make_async_copy(wg_hbm, wg, misc_sem.at[1])
        wu_cp = pltpu.make_async_copy(wu_hbm, wu, misc_sem.at[2])
        wd_cp = pltpu.make_async_copy(wd_hbm, wd, misc_sem.at[3])
        for cp in (res_cp, wg_cp, wu_cp, wd_cp):
            cp.start()

        barrier = pltpu.get_barrier_semaphore()
        for peer in (partner, across, diag):
            pl.semaphore_signal(barrier, inc=1, device_id={"ep": peer}, device_id_type=MESH)
        for peer in (nxt, prv):
            pl.semaphore_signal(barrier, inc=1, device_id={"pp": peer}, device_id_type=MESH)
        pl.semaphore_wait(barrier, 5)

        for rel, peer in ((2, across), (3, diag), (1, partner)):
            meta_copy(rel, peer).start()

        for cp in (res_cp, wg_cp, wu_cp, wd_cp):
            cp.wait()

        def shared(m, carry):
            def norm(k, carry):
                sl = pl.ds(pl.multiple_of(k * piece, piece), piece)
                v = resid[m, sl].astype(F32)
                inv = lax.rsqrt(jnp.mean(v * v, axis=-1, keepdims=True) + EPSILON)
                xs[sl] = (v * inv * norm_moe[...]).astype(BF16)
                return carry

            lax.fori_loop(0, pieces, norm, 0)

            def up(n, carry):
                nn = pl.ds(pl.multiple_of(n * 256, 256), 256)
                g = jnp.dot(xs[...], wg[:, nn], preferred_element_type=F32)
                u = jnp.dot(xs[...], wu[:, nn], preferred_element_type=F32)
                hid[:, nn] = (g * (1.0 / (1.0 + jnp.exp(-g))) * u).astype(BF16)
                return carry

            lax.fori_loop(0, ff // 256, up, 0)
            def down(n, carry):
                nn = pl.ds(pl.multiple_of(n * 256, 256), 256)
                s = jnp.dot(hid[...], wd[:, nn], preferred_element_type=F32).astype(BF16)
                acc[m, :, nn] = resid[m, :, nn].astype(F32) + s.astype(F32)
                return carry

            lax.fori_loop(0, model // 256, down, 0)
            return carry

        lax.fori_loop(0, micro, shared, 0)

        meta_all[0] = meta[...]
        for rel, peer in ((2, across), (3, diag), (1, partner)):
            meta_copy(rel, peer).wait()

        group = 32
        expert = (lax.broadcasted_iota(jnp.int32, (local_experts, half), 0) + local_experts * me).astype(F32)
        lane_slot = (lax.broadcasted_iota(jnp.int32, (group, 256), 1) % cap).astype(F32)
        from_row = lax.broadcasted_iota(jnp.int32, (local_experts, 256), 0)
        to_col = lax.broadcasted_iota(jnp.int32, (local_experts, 256), 1) // cap
        for kb in range(local_cols // 256):
            spread[kb] = jnp.where(from_row == to_col + kb * (256 // cap), 1.0, 0.0).astype(BF16)

        sub = 256 // heads
        mat_blocks = model // D_BLK
        row = lax.broadcasted_iota(jnp.int32, (256, 256), 0)
        col = lax.broadcasted_iota(jnp.int32, (256, 256), 1)
        pick[...] = jnp.where(col == (row % sub) * heads + row // sub, 1.0, 0.0).astype(BF16)

        def in_copy(src, b):
            at = pl.ds(pl.multiple_of(b % mat_blocks * D_BLK, D_BLK), D_BLK)
            return pltpu.make_async_copy(src.at[at], rin.at[b % RIN], rl_in.at[b % RIN])

        def in_start(b):
            for mat, src in enumerate((wq_hbm, wk_hbm, wv_hbm)):
                pl.when(b // mat_blocks == mat)(lambda: in_copy(src, b).start())

        def out_copy(b):
            at = pl.ds(pl.multiple_of(b % mat_blocks * D_BLK, D_BLK), D_BLK)
            return pltpu.make_async_copy(rout.at[b % ROUT], wrel_hbm.at[b // mat_blocks, :, at, :], rl_out.at[b % ROUT])

        for b in range(RIN - RSTEP):
            in_copy(wq_hbm, b).start()

        def gate_table(u):
            u = jnp.minimum(u, 15)
            p, c, ab = u // 4, (u // 2) % 2, u % 2
            rel = (1 - ab) + 2 * (1 - p // 2)
            tab = meta_all[rel, p % 2, :, pl.ds(pl.multiple_of(c * half, half), half)]
            gates, slots = [], []
            for r in range(local_experts // 32):
                ids = expert[r * 32:(r + 1) * 32]
                gate = jnp.zeros((32, half), F32)
                slot = jnp.zeros((32, half), F32)
                for j in range(top_k):
                    hit = tab[j:j + 1] == ids
                    gate = jnp.where(hit, tab[GATE_ROW + j:GATE_ROW + j + 1], gate)
                    slot = jnp.where(hit, tab[SLOT_ROW + j:SLOT_ROW + j + 1], slot)
                gates.append(gate)
                slots.append(slot)
            gate = jnp.concatenate(gates, axis=0).T
            slot = jnp.concatenate(slots, axis=0).T
            hi = jnp.minimum(gate, BF16_MAX).astype(BF16)
            rest = gate - hi.astype(F32)
            mid = rest.astype(BF16)
            low = (rest - mid.astype(F32)).astype(BF16)
            for part, value in enumerate((slot.astype(BF16), hi, mid, low)):
                packed[:, part] = value.reshape(half // group, group, local_experts)

        def spread_group(to, r):
            mix = packed[r].reshape(4 * group, local_experts)
            for kb in range(local_cols // 256):
                wide = jnp.dot(mix, spread[kb], preferred_element_type=F32)
                keep = wide[0:group] == lane_slot
                for part in range(3):
                    term = jnp.where(keep, wide[(part + 1) * group:(part + 2) * group], 0.0)
                    at = pl.ds(pl.multiple_of(part * half + r * group, group), group)
                    wbuf[to, at, kb * 256:(kb + 1) * 256] = term.astype(BF16)

        def first_spread(r, carry):
            spread_group(0, r)
            return carry

        gate_table(0)
        lax.fori_loop(0, half // group, first_spread, 0)
        gate_table(1)

        def partial_sum(p, c, ab, dst, ride=False):
            m = p % 2
            tok = pl.ds(pl.multiple_of(c * half, half), half)

            steps = model // (256 * RSTEP)

            def mul(n, carry):
                b0 = RSTEP * (((2 * p + c - 2) * 2 + ab) * steps + n)
                if ride:
                    for part in range(RSTEP):
                        b = b0 + part
                        in_copy(wq_hbm, b).wait()
                        in_start(b + RIN - RSTEP)
                        pl.when(b >= ROUT)(lambda: out_copy(b - ROUT).wait())
                for part in range(RSTEP):
                    nn = pl.ds(pl.multiple_of((n * RSTEP + part) * 256, 256), 256)
                    rr = rbuf[(2 * p + ab) % 3, :, :, nn].reshape(local_cols, 256)
                    d = jnp.dot(wbuf[ab], rr, preferred_element_type=F32)
                    d = d[0:half] + d[half:2 * half] + d[2 * half:3 * half]
                    dst[m, tok, nn] = dst[m, tok, nn] + d if dst is acc else d
                    if ride:
                        b = b0 + part
                        for i in range(D_BLK // sub):
                            tile = rin[b % RIN, i * sub:(i + 1) * sub].reshape(sub * heads, head_dim)
                            moved = jnp.dot(pick[...], tile, preferred_element_type=F32).astype(BF16)
                            rout[b % ROUT, :, i * sub:(i + 1) * sub, :] = moved.reshape(heads, sub, head_dim)
                    if part % 2 == 1:
                        spread_group(1 - ab, n * (RSTEP // 2) + part // 2)
                if ride:
                    for part in range(RSTEP):
                        out_copy(b0 + part).start()
                return carry

            lax.fori_loop(0, steps, mul, 0)
            gate_table(2 * (2 * p + c) + ab + 2)

        def pair_step(q, ride):
            p, c = q // 2, q % 2
            m = p % 2

            @pl.when(c == 0)
            def _():
                rows_copy(p, 0).wait()
                rows_copy(p, 1).wait()
                pl.when(p < 3)(lambda: rows_copy(p + 1, 0).start())

            pl.when(p >= 2)(lambda: part_copy(m, c).wait_send())
            partial_sum(p, c, 0, send_part, ride)
            pl.when((p < 3) & (c == 1))(lambda: rows_copy(p + 1, 1).start())
            pl.when(p < 2)(lambda: part_copy(m, c).start())
            pl.when(p >= 2)(lambda: own_copy(m, c).start())

            @pl.when(p < 2)
            def _():
                partial_sum(p, c, 1, mine, ride)
                part_copy(m, c).wait_recv()

                def add(k, carry):
                    sl = pl.ds(pl.multiple_of(k * piece, piece), piece)
                    mine[m, sl] = mine[m, sl] + recv_part[m, sl]
                    y_copy(m, k).start()
                    return carry

                lax.fori_loop(c * per_half, (c + 1) * per_half, add, 0)

            if ride:
                pl.when(p >= 2)(lambda: partial_sum(p, c, 1, acc, ride))

        def stage_step(t, carry):
            def riding(c, inner):
                pl.when((t == 3) & (c == 1))(lambda: finish(0, 5, 7))
                pair_step(2 * t + c, True)
                return inner

            lax.fori_loop(0, 2, riding, 0)

            @pl.when(t >= 2)
            def _():
                for c in range(2):
                    own_copy(t - 2, c).wait()
                pl.when(t == 2)(lambda: finish(0, 0, 5))
            return carry

        def first(q, carry):
            pair_step(q, False)
            return carry

        lax.fori_loop(0, 2, first, 0)
        lax.fori_loop(1, 4, stage_step, 0)
        for b in range(3 * mat_blocks - ROUT, 3 * mat_blocks):
            out_copy(b).wait()

    pl.run_scoped(
        phase_one,
        pltpu.VMEM((3, local_experts, cap, model), BF16),
        pltpu.VMEM((2, 3 * half, local_cols), BF16),
        pltpu.VMEM((model, ff), BF16),
        pltpu.VMEM((model, ff), BF16),
        pltpu.VMEM((ff, model), BF16),
        pltpu.VMEM((seq, model), BF16),
        pltpu.VMEM((seq, ff), BF16),
        pltpu.VMEM((micro, seq, model), BF16),
        pltpu.VMEM((local_cols // 256, local_experts, 256), BF16),
        pltpu.VMEM((4, 4, seq // 8, local_experts), BF16),
        pltpu.VMEM((256, 256), BF16),
        pltpu.VMEM((RIN, D_BLK, heads, head_dim), BF16),
        pltpu.VMEM((ROUT, heads, D_BLK, head_dim), BF16),
    )

    def phase_two(wbuf, obuf, wob, xbuf, mixed, qkv):
        def w_copy(g, mat):
            return pltpu.make_async_copy(wrel_hbm.at[mat, g % heads], wbuf.at[g % WSLOTS, mat], w_sem.at[g % WSLOTS, mat])

        n_out = heads * head_dim // OROWS

        def o_copy(n):
            return pltpu.make_async_copy(wo_hbm.at[pl.ds(pl.multiple_of(n * OROWS, OROWS), OROWS)], wob.at[n % OSLOTS], o_sem.at[n % OSLOTS])

        for g in range(WSLOTS - 2):
            for mat in range(3):
                w_copy(g, mat).start()
        for n in range(OSLOTS):
            o_copy(n).start()

        qi = lax.broadcasted_iota(jnp.int32, (seq, seq), 0)
        ki = lax.broadcasted_iota(jnp.int32, (seq, seq), 1)
        causal = qi >= ki
        scale = 1.0 / (head_dim ** 0.5)

        def out_copy(m):
            return pltpu.make_async_copy(obuf, out_hbm.at[m], misc_sem.at[4])

        def attention(m):
            last = m == micro - 1

            def norm(k, carry):
                sl = pl.ds(pl.multiple_of(k * piece, piece), piece)
                z_copy(m, k).wait()
                v = y_in[m, sl].astype(F32)
                inv = lax.rsqrt(jnp.mean(v * v, axis=-1, keepdims=True) + EPSILON)
                xbuf[sl] = (v * inv * norm_attn[...]).astype(BF16)
                return carry

            lax.fori_loop(0, pieces, norm, 0)

            def softmax_head(h, query, key, value, between):
                s = lax.dot_general(query, key, (((1,), (1,)), ((), ())), preferred_element_type=F32) * scale
                between()
                s = jnp.where(causal, s, -1e30)
                e = jnp.exp(s - jnp.max(s, axis=-1, keepdims=True))
                total = jnp.sum(e, axis=-1, keepdims=True)
                between()
                o = jnp.dot(e.astype(BF16), value, preferred_element_type=F32) / total
                between()
                mixed[:, pl.ds(pl.multiple_of(h * head_dim, head_dim), head_dim)] = o.astype(BF16)

            def two_heads(i, carry):
                g = m * heads + 2 * i
                for k in range(2):
                    for mat in range(3):
                        w_copy(g + k, mat).wait()

                def prefetch():
                    for k in range(2):
                        for mat in range(3):
                            w_copy(g + WSLOTS - 2 + k, mat).start()

                if last:
                    pl.when(2 * i + WSLOTS - 2 < heads)(prefetch)
                else:
                    pl.when(2 * i < heads)(prefetch)
                x = xbuf[...]
                fresh = []

                def project():
                    k, mat = len(fresh) // 3, len(fresh) % 3
                    fresh.append(jnp.dot(x, wbuf[(g + k) % WSLOTS, mat], preferred_element_type=F32).astype(BF16))

                softmax_head(jnp.maximum(2 * i - 1, 0), qkv[0], qkv[1], qkv[2], project)
                softmax_head(2 * i, *fresh, project)
                for mat in range(3):
                    qkv[mat] = fresh[3 + mat]
                if not last:
                    pl.when((i % 2 == 0) & (i > 0))(lambda: finish(1, 3 + i // 2, 4 + i // 2))
                return carry

            def proj(n, carry):
                o_copy(n).wait()
                kk = pl.ds(pl.multiple_of(n * OROWS, OROWS), OROWS)
                for j in range(model // 512):
                    nn = slice(j * 512, (j + 1) * 512)
                    part = jnp.dot(mixed[:, kk], wob[n % OSLOTS, :, nn], preferred_element_type=F32)
                    acc[m, :, nn] = jnp.where(n == 0, part, acc[m, :, nn] + part)
                if last:
                    pl.when(n + OSLOTS < n_out)(lambda: o_copy(n + OSLOTS).start())
                else:
                    o_copy((n + OSLOTS) % n_out).start()
                return carry

            lax.fori_loop(0, heads // 2, two_heads, 0)
            if not last:
                finish(1, 7, 8)
            softmax_head(heads - 1, qkv[0], qkv[1], qkv[2], lambda: None)
            lax.fori_loop(0, n_out, proj, 0)

            if m > 0:
                out_copy(m - 1).wait()

            def residual(k, carry):
                sl = pl.ds(pl.multiple_of(k * piece, piece), piece)
                obuf[sl] = (y_in[m, sl].astype(F32) + acc[m, sl].astype(BF16).astype(F32)).astype(BF16)
                return carry

            lax.fori_loop(0, pieces, residual, 0)
            out_copy(m).start()

        qkv[...] = jnp.zeros_like(qkv)
        finish(0, 7, 8)
        finish(1, 0, 4)
        attention(0)
        attention(1)
        out_copy(micro - 1).wait()

    pl.run_scoped(
        phase_two,
        pltpu.VMEM((WSLOTS, 3, model, head_dim), BF16),
        pltpu.VMEM((seq, model), BF16),
        pltpu.VMEM((OSLOTS, OROWS, model), BF16),
        pltpu.VMEM((seq, model), BF16),
        pltpu.VMEM((seq, heads * head_dim), BF16),
        pltpu.VMEM((3, seq, head_dim), BF16),
    )


def solution(mesh):
    stages = mesh.shape["pp"]
    ep_size = mesh.shape["ep"]
    tok_spec = P("pp", "data", "ep", None, None)
    vec_spec = P("pp", None)
    mat_spec = P("pp", None, None)
    head_spec = P("pp", None, None, None)

    def device_step(expert_out, expert_ids, slot_ids, gate_weights, residual, norm_moe, w_gate, w_up, w_down, norm_attn, w_query, w_key, w_value, w_out):
        micro = expert_out.shape[1]
        local_experts, slots_total, model = expert_out.shape[2:]
        cap = slots_total // ep_size
        seq, top_k = expert_ids.shape[3:]
        heads, head_dim = w_query.shape[2:]
        ff = w_gate.shape[2]
        ids = jnp.swapaxes(expert_ids[0, :, 0], 1, 2)
        slots = jnp.swapaxes(slot_ids[0, :, 0], 1, 2)
        gates = jnp.swapaxes(gate_weights[0, :, 0], 1, 2)
        kept = slots >= 0
        experts = jnp.where(kept, ids, -1).astype(F32)
        own_slots = (slots - lax.axis_index("ep") * cap).astype(F32)
        gap = ((0, 0), (0, GATE_ROW - top_k), (0, 0))
        meta = jnp.concatenate([jnp.pad(a, gap) for a in (experts, gates, own_slots)], axis=1)

        dims = (micro, seq, model, heads, head_dim, local_experts, cap, top_k, ff, stages)
        hbm = pl.BlockSpec(memory_space=pl.ANY)
        vmem = pl.BlockSpec(memory_space=pltpu.VMEM)
        dma = pltpu.SemaphoreType.DMA
        pieces = seq // 32
        out, _ = pl.pallas_call(
            functools.partial(boundary_kernel, dims),
            out_shape=(jax.ShapeDtypeStruct((micro, seq, model), BF16), jax.ShapeDtypeStruct((3, heads, model, head_dim), BF16)),
            in_specs=[vmem, hbm, hbm, vmem, vmem] + [hbm] * 7,
            out_specs=(hbm, hbm),
            scratch_shapes=[
                pltpu.VMEM((4, micro, META_ROWS, seq), F32),
                pltpu.VMEM((micro, seq, model), F32),
                pltpu.VMEM((micro, seq, model), F32),
                pltpu.VMEM((micro, seq, model), F32),
                pltpu.VMEM((micro, seq, model), F32),
                pltpu.VMEM((micro, seq, model), F32),
                pltpu.VMEM((micro, seq, model), F32),
                pltpu.VMEM((micro, seq, model), BF16),
                pltpu.VMEM((micro, seq, model), BF16),
                dma((3,)), dma((3,)),
                dma((micro, 2)), dma((micro, 2)),
                dma((micro, 2)), dma((micro, 2)),
                dma((micro, pieces)), dma((micro, pieces)),
                dma((micro, pieces)), dma((micro, pieces)),
                dma((3,)), dma((5,)), dma((WSLOTS, 3)), dma((OSLOTS,)), dma((RIN,)), dma((ROUT,)),
            ],
            compiler_params=pltpu.CompilerParams(collective_id=0, has_side_effects=True, vmem_limit_bytes=67043328),
        )(
            meta,
            expert_out[0],
            residual[0, :, 0],
            norm_moe, norm_attn,
            w_gate[0], w_up[0], w_down[0],
            w_query[0], w_key[0], w_value[0],
            w_out[0].reshape(heads * head_dim, model),
        )
        return out[None, :, None]

    in_specs = (tok_spec,) * 5 + (vec_spec, mat_spec, mat_spec, mat_spec, vec_spec, head_spec, head_spec, head_spec, head_spec)
    return jax.shard_map(device_step, mesh=mesh, in_specs=in_specs, out_specs=tok_spec, check_vma=False)
```
